32 devices in a mesh: fft: 16 (over z, x, core), scal: 2 (over y).
Axes of the slice: x: 2, y: 2, z: 4, core: 2. Of those that a mesh axis runs over, the one named last changes fastest.
Arguments:
- scalar_state: float32 [2, 2, 256, 256, 128], P('scal', None, 'fft'), may hold values from -12 to 12
- velocity: bfloat16 [3, 256, 256, 256], P(None, 'fft', 'scal'), may hold values from -6 to 6
- species: int32 [2], P('scal'), may hold values from 0 to 63
- kappa_table: float32 [64], replicated, may hold values from 0.1 to 1
- dealias_bound: int32 [2], P('scal'), may hold values from 64 to 85
Outputs:
- new_state: float32 [2, 2, 256, 256, 128], P('scal', None, 'fft')
- kappa: float32 [2], P('scal')
The draws below stay inside these ranges and needn't reach their ends.
All inputs are finite; a program needn't handle non-finite values.
Results may differ from the reference program's by a relative error of at most 0.0027.
Values may be sent and summed in bfloat16 or wider, within the bound.
A program may use at most 128 MiB of HBM per device.

```python
import math
import jax
import jax.numpy as jnp
from jax import lax

N = 256
SPECIES = 64
SCALARS = 2


def draw_scalar_state(key, part):
    dims_shape = (SCALARS, 2, N, N, N // 2)
    key_base, key_rough, key_scale = jax.random.split(key, 3)
    values = jnp.clip(jax.random.normal(key_base, dims_shape, jnp.float32), -4.0, 4.0)
    roughness = jnp.exp(jax.random.uniform(key_rough, dims_shape, jnp.float32, math.log(0.5), math.log(1.5)))
    ky_float = jnp.arange(N, dtype=jnp.int32).astype(jnp.float32)
    envelope = jnp.sqrt(1.0 + 2.0 * ky_float / (N - 1)).reshape(1, 1, N, 1, 1)
    scalar_scale = jnp.exp(jax.random.uniform(key_scale, (SCALARS, 1, 1, 1, 1), jnp.float32, math.log(0.5), math.log(2.0)))
    return jnp.clip(values * roughness * envelope * scalar_scale, -12.0, 12.0).astype(jnp.float32)


def block_scale(rng, dims, cuts, least, largest):
    loudness, own = 1.0, jax.random.fold_in(rng, 6)
    for position, shards_of in cuts:
        heights = jnp.exp(jax.random.uniform(jax.random.fold_in(own, position), (shards_of,), jnp.float32, least / len(cuts), largest / len(cuts)))
        loudness = loudness * jnp.repeat(heights, dims[position] // shards_of).reshape([-1 if axis == position else 1 for axis in range(len(dims))])
    return loudness


def noise(stream_key, shape, spread, most, cuts=(), kind=jnp.bfloat16):
    entries = jax.random.normal(stream_key, shape, jnp.float32) * spread
    if len(cuts) > 0:
        entries = block_scale(stream_key, shape, cuts, -0.22, 0.18) * entries
    return jnp.clip(entries, min=-most, max=most).astype(kind)


def setup_inputs(seed: int = 0) -> dict:
    keys = jax.random.split(jax.random.key(seed), 6)
    return {
        "scalar_state": draw_scalar_state(jax.random.fold_in(keys[5], 71), 0),
        "velocity": noise(keys[1], (3, N, N, N), 1.0, 6.0, ((1, 16), (2, 2))),
        "species": jax.random.randint(keys[2], (SCALARS,), 0, SPECIES).astype(jnp.int32),
        "kappa_table": jnp.clip(jnp.exp(jax.random.uniform(keys[3], (SPECIES,), jnp.float32, math.log(0.1), math.log(1.0))), 0.1, 1.0),
        "dealias_bound": jax.random.randint(keys[4], (SCALARS,), N // 4, N // 3 + 1).astype(jnp.int32),
    }


cfl_number = 0.2

def twiddle(size_in, size_out, length):
    row_index = jnp.arange(size_in, dtype=jnp.int32)[:, None]
    col_index = jnp.arange(size_out, dtype=jnp.int32)[None, :]
    angles = (row_index * col_index % length).astype(jnp.float32) * (2.0 * math.pi / length)
    norming = 1.0 / math.sqrt(length)
    return (jnp.cos(angles) * norming, jnp.sin(angles) * norming)

def build_tables(length):
    half_len = length // 2
    full_cos, full_sin = twiddle(length, length, length)
    inv_cos, inv_sin = twiddle(half_len, length, length)
    weight = jnp.where(jnp.arange(half_len, dtype=jnp.int32) == 0, 1.0, 2.0).astype(jnp.float32)[:, None]
    fwd_cos, fwd_sin = twiddle(length, half_len, length)
    listed = (full_cos, full_sin, inv_cos * weight, inv_sin * weight, fwd_cos, fwd_sin)
    return tuple((matrix.astype(jnp.bfloat16) for matrix in listed))

def product(formula, operand, matrix):
    return jnp.einsum(formula, operand.astype(jnp.float32), matrix.astype(jnp.float32), precision=lax.Precision.HIGHEST)

def complex_section(real_part, imag_part, cos_matrix, sin_matrix, formula, inverse):
    real_cos = product(formula, real_part, cos_matrix)
    real_sin = product(formula, real_part, sin_matrix)
    imag_cos = product(formula, imag_part, cos_matrix)
    imag_sin = product(formula, imag_part, sin_matrix)
    if inverse:
        return (real_cos - imag_sin, real_sin + imag_cos)
    return (real_cos + imag_sin, imag_cos - real_sin)

def reference(scalar_state, velocity, species, kappa_table, dealias_bound):
    scalar_count = scalar_state.shape[0]
    table_count = kappa_table.shape[0]
    length = scalar_state.shape[2]
    half_len = length // 2
    full_cos, full_sin, inv_cos, inv_sin, fwd_cos, fwd_sin = build_tables(length)
    index_full = jnp.arange(length, dtype=jnp.int32)
    signed = jnp.where(index_full < half_len, index_full, index_full - length).astype(jnp.float32)
    ky_wave = signed[:, None, None]
    kz_wave = signed[None, :, None]
    kx_wave = jnp.arange(half_len, dtype=jnp.int32).astype(jnp.float32)[None, None, :]
    ksquare = kx_wave * kx_wave + ky_wave * ky_wave + kz_wave * kz_wave
    weight = jnp.where(kx_wave == 0.0, 1.0, 2.0).astype(jnp.float32)
    cell_count = float(length) ** 3
    step_size = cfl_number * 2.0 * math.pi / length

    def z_inverse(real_part, imag_part):
        z_section = complex_section(real_part, imag_part, full_cos, full_sin, 'ykx,kz->yzx', True)
        return (z_section[0].astype(jnp.bfloat16), z_section[1].astype(jnp.bfloat16))

    def rest_inverse(real_part, imag_part):
        y_section = complex_section(real_part, imag_part, full_cos, full_sin, 'yzx,yw->zwx', True)
        y_real = y_section[0].astype(jnp.bfloat16)
        y_imag = y_section[1].astype(jnp.bfloat16)
        return product('zwk,kx->zwx', y_real, inv_cos) - product('zwk,kx->zwx', y_imag, inv_sin)

    def gradient_set(real_part, imag_part):
        whole_real, whole_imag = z_inverse(real_part.astype(jnp.bfloat16), imag_part.astype(jnp.bfloat16))
        deriv_real, deriv_imag = z_inverse((-kz_wave * imag_part).astype(jnp.bfloat16), (kz_wave * real_part).astype(jnp.bfloat16))
        results = []
        for wavenumber in (kx_wave, ky_wave):
            grad_real = (-wavenumber * whole_imag.astype(jnp.float32)).astype(jnp.bfloat16)
            grad_imag = (wavenumber * whole_real.astype(jnp.float32)).astype(jnp.bfloat16)
            results.append(rest_inverse(grad_real, grad_imag))
        results.append(rest_inverse(deriv_real, deriv_imag))
        return results

    def advect(gradients):
        total = velocity[0].astype(jnp.float32) * gradients[0]
        total = total + velocity[1].astype(jnp.float32) * gradients[1]
        total = total + velocity[2].astype(jnp.float32) * gradients[2]
        return total.astype(jnp.bfloat16)

    def forward_field(physical):
        real_x = product('zyx,xk->zyk', physical, fwd_cos).astype(jnp.bfloat16)
        imag_x = (-product('zyx,xk->zyk', physical, fwd_sin)).astype(jnp.bfloat16)
        y_section = complex_section(real_x, imag_x, full_cos, full_sin, 'zyk,yw->wzk', False)
        y_real = y_section[0].astype(jnp.bfloat16)
        y_imag = y_section[1].astype(jnp.bfloat16)
        return complex_section(y_real, y_imag, full_cos, full_sin, 'wzk,zv->wvk', False)
    updated_list = []
    kappa_list = []
    for scalar in range(scalar_count):
        start_real = scalar_state[scalar, 0]
        start_imag = scalar_state[scalar, 1]
        energy = start_real * start_real + start_imag * start_imag
        variance = jnp.sum(weight * energy) / cell_count
        mean_grad = jnp.sum(weight * ksquare * energy) / cell_count
        gradients = gradient_set(start_real, start_imag)
        peak_value = jnp.max(jnp.sqrt(gradients[0] * gradients[0] + gradients[1] * gradients[1] + gradients[2] * gradients[2]))
        base_kappa = jnp.sum(jnp.where(species[scalar] == jnp.arange(table_count, dtype=jnp.int32), kappa_table, 0.0))
        kappa_value = base_kappa * peak_value * jnp.sqrt(variance) / (mean_grad + 1e-06)
        factor = jnp.exp(-kappa_value * ksquare * step_size)
        bound = dealias_bound[scalar].astype(jnp.float32)
        dealias_mask = (ksquare <= bound * bound).astype(jnp.float32)
        first_real, first_imag = forward_field(advect(gradients))
        first_real = -dealias_mask * first_real
        first_imag = -dealias_mask * first_imag
        mid_real = factor * (start_real + step_size * first_real)
        mid_imag = factor * (start_imag + step_size * first_imag)
        second_real, second_imag = forward_field(advect(gradient_set(mid_real, mid_imag)))
        second_real = -dealias_mask * second_real
        second_imag = -dealias_mask * second_imag
        new_real = factor * start_real + 0.5 * step_size * (factor * first_real + second_real)
        new_imag = factor * start_imag + 0.5 * step_size * (factor * first_imag + second_imag)
        updated_list.append(jnp.stack([new_real, new_imag]))
        kappa_list.append(kappa_value)
    return (jnp.stack(updated_list), jnp.stack(kappa_list))
```

```python
import functools
import math

import numpy as np

import jax
import jax.numpy as jnp
from jax import lax
from jax.experimental import pallas as pl
from jax.experimental.pallas import tpu as pltpu
from jax.sharding import PartitionSpec as P

MESH = pl.DeviceIdType.MESH
cfl_number = 0.2
CHUNK = 4


def twiddle(size_in, size_out, length):
    row_index = np.arange(size_in, dtype=np.int32)[:, None]
    col_index = np.arange(size_out, dtype=np.int32)[None, :]
    angles = (row_index * col_index % length).astype(np.float32) * np.float32(2.0 * math.pi / length)
    norming = np.float32(1.0 / math.sqrt(length))
    return (np.cos(angles) * norming, np.sin(angles) * norming)


def build_tables(length, n, rows):
    half = length // 2
    quarter = half // 4
    sides = n // 2
    full_cos, full_sin = twiddle(length, length, length)
    inv_cos, inv_sin = twiddle(half, length, length)
    weight = np.where(np.arange(half) == 0, 1.0, 2.0).astype(np.float32)[:, None]
    fwd_cos, fwd_sin = twiddle(length, half, length)
    inv_z = np.block([[full_cos[:half], -full_sin[:half]], [full_sin[:half], full_cos[:half]]])
    inv_y = np.block([[full_cos, -full_sin], [full_sin, full_cos]])
    q, h, c, p, k = np.meshgrid(
        np.arange(sides), np.arange(2), np.arange(rows // CHUNK), np.arange(2), np.arange(CHUNK), indexing="ij"
    )
    inv_y = inv_y[:, ((q + h * sides) * rows + c * CHUNK + k + p * length).reshape(-1)]
    inv_x = np.concatenate([inv_cos * weight, -inv_sin * weight], axis=0)
    orders = [
        np.concatenate([((p - l - 1) % 4) * quarter + np.arange(quarter) for l in range(4)]) for p in range(4)
    ]
    fwd_x = np.stack([np.concatenate([fwd_cos[:, o], -fwd_sin[:, o]], axis=1) for o in orders])
    fwd_y = np.block([[full_cos, full_sin], [-full_sin, full_cos]])
    z, s, p = np.meshgrid(np.arange(rows), np.arange(n), np.arange(2), indexing="ij")
    fwd_z = fwd_y[:, (s * rows + z + p * length).reshape(-1)]
    return tuple(
        jnp.asarray(t.astype(np.float32).astype(jnp.bfloat16)) for t in (inv_z, inv_y, inv_x, fwd_x, fwd_y, fwd_z)
    )


def dot(a, b):
    return jnp.dot(a, b, preferred_element_type=jnp.float32)


def step_kernel(n, m, rows, band, *refs):
    (state, vel, species, ktable, bounds, inv_z, inv_y, inv_x, fwd_x, fwd_y, fwd_z,
     out, kap,
     tb, wsend, recv, tmp, uall, fsend, raw, packed, tf, zin, iny, inx, peak, acc, stat, stats,
     s_load, x_send, x_recv, w_send, w_recv, w_loc, u_send, u_recv, u_loc,
     f_send, f_recv, f_loc, t_send, t_recv, t_loc, free) = refs
    length = n * rows
    half = length // 2
    quarter = half // 4
    sides = n // 2
    nch = rows // CHUNK
    groups = rows // 4
    f32 = jnp.float32
    bf16 = jnp.bfloat16
    step_size = cfl_number * 2.0 * math.pi / length
    cells = float(length) ** 3
    me = lax.axis_index("fft")
    mine = lax.axis_index("scal")
    side = me // sides
    place = me % sides
    partner = (me + sides) % n

    def each(low, high, act):
        def one(j, carry):
            act(j)
            return carry

        lax.fori_loop(low, high, one, 0)

    def load_copy(c):
        at = pl.ds(c * CHUNK, CHUNK)
        return pltpu.make_async_copy(state.at[:, at], out.at[:, at], s_load.at[c])

    def swap_copy(c, h):
        at = pl.ds(c * CHUNK, CHUNK)
        return pltpu.make_async_remote_copy(
            src_ref=tb.at[h, at], dst_ref=tb.at[h, at], send_sem=x_send.at[c], recv_sem=x_recv.at[c],
            device_id={"fft": partner}, device_id_type=MESH,
        )

    def row_copy(st, h, c, to, slot):
        return pltpu.make_async_remote_copy(
            src_ref=wsend.at[h, c, to], dst_ref=recv.at[slot, h, c],
            send_sem=w_send.at[st, h, c, to], recv_sem=w_recv.at[st, h, c, slot],
            device_id={"fft": side * sides + to}, device_id_type=MESH,
        )

    def own_row(st, h, c):
        return pltpu.make_async_copy(wsend.at[h, c, place], recv.at[place, h, c], w_loc.at[st, h, c])

    def speed_copy(g, s, slot):
        at = pl.ds(g * 4, 4)
        return pltpu.make_async_remote_copy(
            src_ref=vel.at[:, at], dst_ref=uall.at[:, at, slot],
            send_sem=u_send.at[g, s], recv_sem=u_recv.at[g, slot],
            device_id={"scal": s}, device_id_type=MESH,
        )

    def own_speed(g):
        at = pl.ds(g * 4, 4)
        return pltpu.make_async_copy(vel.at[:, at], uall.at[:, at, mine], u_loc.at[g])

    def forward_copy(st, g, d, h, slot, k):
        return pltpu.make_async_remote_copy(
            src_ref=fsend.at[d % sides + h * sides, g, pl.ds(0, k)], dst_ref=raw.at[h, slot, g, pl.ds(0, k)],
            send_sem=f_send.at[st, g, h, d], recv_sem=f_recv.at[st, g, h, slot],
            device_id={"fft": d}, device_id_type=MESH,
        )

    def own_forward(st, g, h):
        return pltpu.make_async_copy(fsend.at[place + h * sides, g], raw.at[h, me, g], f_loc.at[st, g, h])

    def stat_copy(d, slot):
        return pltpu.make_async_remote_copy(
            src_ref=stat, dst_ref=stats.at[slot], send_sem=t_send.at[d], recv_sem=t_recv.at[slot],
            device_id={"fft": d}, device_id_type=MESH,
        )

    def needed(b, t):
        low = b * rows
        least = jnp.where(low < half, low, length - low - rows + 1)
        return (t * quarter) ** 2 + least * least <= band * band

    def by_tiles(b, act):
        for k in range(1, 4):
            wanted = needed(b, k - 1)
            if k < 3:
                wanted = jnp.logical_and(wanted, jnp.logical_not(needed(b, k)))

            @pl.when(wanted)
            def _():
                act(k)

    def chunk_inside(h, c):
        low = (place + h * sides) * rows + c * CHUNK
        least = jnp.where(low < half, low, length - low - CHUNK + 1)
        return least <= band

    each(0, nch, lambda c: load_copy(c).start())

    barrier = pltpu.get_barrier_semaphore()
    each(1, n, lambda j: pl.semaphore_signal(
        barrier, inc=1, device_id={"fft": (me + j) % n}, device_id_type=MESH))
    each(1, m, lambda j: pl.semaphore_signal(
        barrier, inc=1, device_id={"scal": (mine + j) % m}, device_id_type=MESH))

    lane = lax.broadcasted_iota(jnp.int32, (half, 2 * length), 1) % length
    flip = jnp.where((lane % 2) * side == 1, -1.0, 1.0)
    kz_lane = jnp.where(lane < half, lane, lane - length).astype(f32)
    real_z = inv_z[:half].astype(f32) * flip
    imag_z = inv_z[half:].astype(f32) * flip
    zin[0:half] = real_z.astype(bf16)
    zin[half:length] = imag_z.astype(bf16)
    zin[length:length + half] = (-kz_lane * imag_z).astype(bf16)
    zin[length + half:] = (kz_lane * real_z).astype(bf16)

    pl.semaphore_wait(barrier, n + m - 2)

    def start_speed(g):
        each(1, m, lambda j: speed_copy(g, (mine + j) % m, mine).start())
        own_speed(g).start()

    def z_pair(pr, pair):
        res = dot(zin[...], pair)
        for k in range(2):
            for f in range(2):
                for p in range(2):
                    at = f * length + p * half
                    tmp[f, pl.ds(p * CHUNK + 2 * pr + k, half, stride=2 * CHUNK), :] = (
                        res[at:at + half, k * half:(k + 1) * half]
                    )

    def send_rows(st, h, c):
        both = jnp.concatenate([tmp[0].astype(bf16), tmp[1].astype(bf16)], axis=1)
        wsend[h, c] = both.reshape(sides, rows, 2 * CHUNK, 2 * half)
        each(1, sides, lambda j: row_copy(st, h, c, (place + j) % sides, place).start())
        own_row(st, h, c).start()

    def begin(i):
        c = i % nch
        own = i < nch
        h = jnp.where(own, side, 1 - side)

        @pl.when(own)
        def _():
            load_copy(c).wait()

            def cast(r):
                tb[side, r] = out[:, r].astype(bf16)

            each(c * CHUNK, c * CHUNK + CHUNK, cast)
            swap_copy(c, side).start()

        @pl.when(jnp.logical_not(own))
        def _():
            swap_copy(c, 1 - side).wait_recv()

        def pair(pr):
            r = c * CHUNK + 2 * pr
            z_pair(pr, jnp.concatenate(
                [tb[h, r].reshape(2 * length, half), tb[h, r + 1].reshape(2 * length, half)], axis=1))

        each(0, CHUNK // 2, pair)
        send_rows(0, h, c)

    each(0, nch, begin)
    each(0, groups, start_speed)

    kx = lax.broadcasted_iota(jnp.int32, (length, half), 1).astype(f32)
    kz_row = lax.broadcasted_iota(jnp.int32, (length, half), 0)
    kz = jnp.where(kz_row < half, kz_row, kz_row - length).astype(f32)
    kxz = kx * kx + kz * kz
    weight = jnp.where(kx == 0.0, 1.0, 2.0)

    def ky_square(b, r):
        index = b * rows + r
        wave = jnp.where(index < half, index, index - length)
        return jnp.full((1, half), wave * wave, jnp.int32).astype(f32)

    acc[...] = jnp.zeros_like(acc)

    def add_row(r):
        real, imag = out[0, r], out[1, r]
        energy = weight * (real * real + imag * imag)
        acc[0] += jnp.sum(energy.reshape(length // 8, 8, half), axis=0)
        acc[1] += jnp.sum((energy * (kxz + ky_square(me, r))).reshape(length // 8, 8, half), axis=0)

    each(0, rows, add_row)

    col = lax.broadcasted_iota(jnp.int32, (length, 2 * length), 1)
    row_ky = ((col // (2 * CHUNK * nch * 2)) + ((col // (2 * CHUNK * nch)) % 2) * sides) * rows
    row_ky = row_ky + ((col // (2 * CHUNK)) % nch) * CHUNK + col % CHUNK
    row_ky = jnp.where(row_ky < half, row_ky, row_ky - length).astype(f32)
    iny[:length] = (-row_ky * inv_y[length:].astype(f32)).astype(bf16)
    iny[length:] = (row_ky * inv_y[:length].astype(f32)).astype(bf16)
    kx_row = lax.broadcasted_iota(jnp.int32, (half, length), 0).astype(f32)
    inx[:half] = (kx_row * inv_x[half:].astype(f32)).astype(bf16)
    inx[half:] = (-kx_row * inv_x[:half].astype(f32)).astype(bf16)

    for h in range(2):
        for t in range(3):
            @pl.when(jnp.logical_not(needed(place + h * sides, t)))
            def _():
                def clear(j):
                    raw[h, (me + j) % n, :, t] = jnp.zeros((groups, 2, rows, half), bf16)

                each(1, n, clear)

    peak[...] = jnp.zeros_like(peak)

    each(nch, 2 * nch, begin)

    tile_lane = lax.broadcasted_iota(jnp.int32, (2 * length, half), 1) // quarter

    def pick(choices):
        result = choices[-1]
        for i in range(len(choices) - 2, -1, -1):
            result = jnp.where(tile_lane == i, choices[i], result)
        return result

    def pair_planes(st, z, hh):
        blocks = [recv[:, :, :, z + p].reshape(2 * length, 2 * half) for p in range(2)]
        section = dot(inv_y[...], jnp.concatenate(blocks, axis=1)).astype(bf16)
        turned = dot(iny[...], jnp.concatenate([b[:, :half] for b in blocks], axis=1)).astype(bf16)
        halves = []
        for p in range(2):
            at = 2 * half * p
            sides_of = [
                (section[:, at:at + half], inx),
                (turned[:, half * p:half * (p + 1)], inv_x),
                (section[:, at + half:at + 2 * half], inv_x),
            ]
            total = None
            square = None
            for i, (part, table) in enumerate(sides_of):
                lhs = jnp.concatenate([part[:length], part[length:]], axis=1)
                grad = dot(lhs, table[...])
                u = uall[i, z + p].reshape(length, length).astype(f32)
                total = u * grad if total is None else total + u * grad
                if st == 0:
                    square = grad * grad if square is None else square + grad * grad
            if st == 0:
                peak[...] = jnp.maximum(peak[...], jnp.max(square.reshape(length // 8, 8, length), axis=0))
            flat = dot(total.astype(bf16), fwd_x[2 * hh + p]).astype(bf16)
            halves.append(jnp.concatenate([flat[:, :half], flat[:, half:]], axis=0))
        packed[hh] = dot(fwd_y[...], jnp.concatenate(halves, axis=1))

    def physical(st):
        def arrive(h):
            def chunk(c):
                each(1, sides, lambda j: row_copy(
                    st, h, c, (place + j) % sides, (place + sides - j) % sides).wait_recv())
                own_row(st, h, c).wait()

            each(0, nch, chunk)

        each(0, 2, arrive)
        if st == 0:
            def arrive_speed(g):
                each(1, m, lambda j: speed_copy(g, (mine + j) % m, (mine + m - j) % m).wait_recv())
                own_speed(g).wait()

            each(0, groups, arrive_speed)

        def run_group(g):
            for hh in range(2):
                pair_planes(st, g * 4 + 2 * hh, hh)
            for t in range(3):
                chosen = [(i + 1 + t) % 4 for i in range(4)]
                tile = pick([packed[p // 2, :, (p % 2) * half:(p % 2 + 1) * half] for p in chosen]).astype(bf16)
                for q in range(2):
                    fsend[:, g, t, q] = tile[q * length:(q + 1) * length].reshape(n, rows, half)
            if st == 1:
                @pl.when(g == 0)
                def _():
                    pl.semaphore_wait(free, n - 1)

            def leave(j):
                d = (me + j) % n
                for_blocks(st, d, lambda h: by_tiles(
                    d % sides + h * sides, lambda k: forward_copy(st, g, d, h, me, k).start()))

            each(1, n, leave)
            for_blocks(st, me, lambda h: own_forward(st, g, h).start())

        each(0, groups, run_group)

    def for_blocks(st, d, act):
        if st == 0:
            each(0, 2, act)
        else:
            act(d // sides)

    def forward_arrive(st, h):
        def group(g):
            each(1, n, lambda j: by_tiles(place + h * sides, lambda k: forward_copy(
                st, g, (me + j) % n, h, (me + n - j) % n, k).wait_recv()))
            own_forward(st, g, h).wait()

        each(0, groups, group)

    def forward_sent(st):
        def group(g):
            def one(j):
                d = (me + j) % n
                for_blocks(st, d, lambda h: by_tiles(
                    d % sides + h * sides, lambda k: forward_copy(st, g, d, h, me, k).wait_send()))

            each(1, n, one)

        each(0, groups, group)

    def rows_sent(st):
        each(0, 2, lambda h: each(0, nch, lambda c: each(
            1, sides, lambda j: row_copy(st, h, c, (place + j) % sides, place).wait_send())))

    def unpack(h):
        def group(g):
            tiles = [raw[h, :, g, t].reshape(2 * length, half).astype(f32) for t in range(3)]
            for p in range(4):
                moved = [
                    pltpu.roll(tiles[t], (2 * t + 1 - p) % 4 * quarter, 1) if (2 * t + 1 - p) % 4 else tiles[t]
                    for t in range(3)
                ]
                at = pl.multiple_of((4 * g + p) * 2 * length, 2 * length)
                tf[pl.ds(at, 2 * length), :] = pick(moved + [jnp.zeros_like(tiles[0])])

        each(0, groups, group)

    def z_forward(r):
        pair = [tf[pl.ds(r + k, 2 * length, stride=rows), :].astype(bf16) for k in range(2)]
        return dot(fwd_z[...], jnp.concatenate(pair, axis=1))

    physical(0)

    line = lax.broadcasted_iota(jnp.int32, (8, 128), 0)
    largest = jnp.sqrt(jnp.max(peak[...], keepdims=True))
    local_var = jnp.sum(acc[0], keepdims=True) / cells
    local_grad = jnp.sum(acc[1], keepdims=True) / cells
    stat[...] = jnp.where(line == 0, local_var, jnp.where(line == 1, local_grad, largest))
    each(1, n, lambda j: stat_copy((me + j) % n, me).start())
    stats[me] = stat[...]
    rows_sent(0)
    each(1, n, lambda j: stat_copy((me + j) % n, (me + n - j) % n).wait_recv())
    summed = jnp.sum(stats[...], axis=0)
    highest = jnp.max(stats[...], axis=0)
    kappa = ktable[species[0]] * highest[2:3, :1] * jnp.sqrt(summed[0:1, :1]) / (summed[1:2, :1] + 1e-06)
    kap[...] = jnp.broadcast_to(kappa, kap.shape)
    bound = jnp.full((1, half), bounds[0], jnp.int32).astype(f32)
    bound = bound * bound
    rate = -kappa * step_size

    def second(h, c, inside):
        block = place + h * sides

        def pair(pr):
            r = c * CHUNK + 2 * pr
            moved = z_forward(r) if inside else None
            cols = []
            for k in range(2):
                square = kxz + ky_square(block, r + k)
                factor = jnp.exp(rate * square)
                real = tb[h, r + k, 0].astype(f32)
                imag = tb[h, r + k, 1].astype(f32)
                if inside:
                    keep = square <= bound
                    add_real = jnp.where(keep, -step_size * moved[:length, k * half:(k + 1) * half], 0.0)
                    add_imag = jnp.where(keep, -step_size * moved[length:, k * half:(k + 1) * half], 0.0)
                    real = real + add_real
                    imag = imag + add_imag
                cols.append(jnp.concatenate([(factor * real).astype(bf16), (factor * imag).astype(bf16)], axis=0))

                @pl.when(h == side)
                def _():
                    if inside:
                        out[0, r + k] = factor * (out[0, r + k] + 0.5 * add_real)
                        out[1, r + k] = factor * (out[1, r + k] + 0.5 * add_imag)
                    else:
                        out[0, r + k] = factor * out[0, r + k]
                        out[1, r + k] = factor * out[1, r + k]

            z_pair(pr, jnp.concatenate(cols, axis=1))

        each(0, CHUNK // 2, pair)
        send_rows(1, h, c)

    def early(i):
        h, c = i // nch, i % nch

        @pl.when(jnp.logical_not(chunk_inside(h, c)))
        def _():
            second(h, c, False)

    each(0, 2 * nch, early)

    def late(i):
        h = (side + i) % 2
        forward_arrive(0, h)
        unpack(h)

        @pl.when(i == 1)
        def _():
            each(1, n, lambda j: pl.semaphore_signal(
                free, inc=1, device_id={"fft": (me + j) % n}, device_id_type=MESH))

        def chunk(c):
            @pl.when(chunk_inside(h, c))
            def _():
                second(h, c, True)

        each(0, nch, chunk)

    each(0, 2, late)
    forward_sent(0)
    physical(1)
    forward_arrive(1, side)
    unpack(side)

    def finish(c):
        @pl.when(chunk_inside(side, c))
        def _():
            def pair(pr):
                r = c * CHUNK + 2 * pr
                moved = z_forward(r)
                for k in range(2):
                    keep = kxz + ky_square(me, r + k) <= bound
                    for p in range(2):
                        value = moved[p * length:(p + 1) * length, k * half:(k + 1) * half]
                        out[p, r + k] += jnp.where(keep, -0.5 * step_size * value, 0.0)

            each(0, CHUNK // 2, pair)

    each(0, nch, finish)

    each(0, nch, lambda c: swap_copy(c, side).wait_send())
    each(0, groups, lambda g: each(1, m, lambda j: speed_copy(g, (mine + j) % m, mine).wait_send()))
    each(1, n, lambda j: stat_copy((me + j) % n, me).wait_send())
    rows_sent(1)
    forward_sent(1)


def body(n, m, scalar_state, velocity, species, kappa_table, dealias_bound):
    rows = scalar_state.shape[2]
    length = scalar_state.shape[3]
    half = length // 2
    sides = n // 2
    nch = rows // CHUNK
    groups = rows // 4
    f32, bf16 = jnp.float32, jnp.bfloat16
    tables = lax.optimization_barrier(build_tables(length, n, rows))
    vmem = pl.BlockSpec(memory_space=pltpu.VMEM)
    smem = pl.BlockSpec(memory_space=pltpu.SMEM)
    hbm = pl.BlockSpec(memory_space=pl.ANY)
    dma = pltpu.SemaphoreType.DMA
    scratch = [
        pltpu.VMEM((2, rows, 2, length, half), bf16),
        pltpu.VMEM((2, nch, sides, rows, 2 * CHUNK, 2 * half), bf16),
        pltpu.VMEM((sides, 2, nch, rows, 2 * CHUNK, 2 * half), bf16),
        pltpu.VMEM((2, half * 2 * CHUNK, half), f32),
        pltpu.VMEM((3, rows, m, length // m, length), bf16),
        pltpu.VMEM((n, groups, 3, 2, rows, half), bf16),
        pltpu.VMEM((2, n, groups, 3, 2, rows, half), bf16),
        pltpu.VMEM((2, 2 * length, 2 * half), f32),
        pltpu.VMEM((rows * 2 * length, half), f32),
        pltpu.VMEM((2 * length, 2 * length), bf16),
        pltpu.VMEM((2 * length, 2 * length), bf16),
        pltpu.VMEM((length, length), bf16),
        pltpu.VMEM((8, length), f32),
        pltpu.VMEM((2, 8, half), f32),
        pltpu.VMEM((8, 128), f32),
        pltpu.VMEM((n, 8, 128), f32),
        dma((nch,)), dma((nch,)), dma((nch,)),
        dma((2, 2, nch, sides)), dma((2, 2, nch, sides)), dma((2, 2, nch)),
        dma((groups, m)), dma((groups, m)), dma((groups,)),
        dma((2, groups, 2, n)), dma((2, groups, 2, n)), dma((2, groups, 2)),
        dma((n,)), dma((n,)), dma,
        pltpu.SemaphoreType.REGULAR,
    ]
    new_state, kappa = pl.pallas_call(
        functools.partial(step_kernel, n, m, rows, length // 3),
        out_shape=[
            jax.ShapeDtypeStruct((2, rows, length, half), f32),
            jax.ShapeDtypeStruct((8, 128), f32),
        ],
        in_specs=[hbm, hbm, smem, smem, smem] + [vmem] * 6,
        out_specs=[vmem, vmem],
        scratch_shapes=scratch,
        compiler_params=pltpu.CompilerParams(
            collective_id=0, has_side_effects=True, vmem_limit_bytes=63 * 1024 * 1024,
        ),
        name="whole_step",
    )(scalar_state[0], velocity, species, kappa_table, dealias_bound, *tables)
    return new_state[None], kappa[0, :1]


def solution(mesh):
    placed = (
        P("scal", None, "fft", None, None),
        P(None, "fft", "scal", None),
        P("scal"),
        P(),
        P("scal"),
    )
    return jax.shard_map(
        functools.partial(body, mesh.shape["fft"], mesh.shape["scal"]),
        mesh=mesh,
        in_specs=placed,
        out_specs=(P("scal", None, "fft", None, None), P("scal")),
        check_vma=False,
    )
```

```python
import functools
import math

import numpy as np

import jax
import jax.numpy as jnp
from jax import lax
from jax.experimental import pallas as pl
from jax.experimental.pallas import tpu as pltpu
from jax.sharding import PartitionSpec as P

MESH = pl.DeviceIdType.MESH
cfl_number = 0.2
CHUNK = 4


def twiddle(size_in, size_out, length):
    row_index = np.arange(size_in, dtype=np.int32)[:, None]
    col_index = np.arange(size_out, dtype=np.int32)[None, :]
    angles = (row_index * col_index % length).astype(np.float32) * np.float32(2.0 * math.pi / length)
    norming = np.float32(1.0 / math.sqrt(length))
    return (np.cos(angles) * norming, np.sin(angles) * norming)


def build_tables(length, n, rows):
    half = length // 2
    quarter = half // 4
    sides = n // 2
    full_cos, full_sin = twiddle(length, length, length)
    inv_cos, inv_sin = twiddle(half, length, length)
    weight = np.where(np.arange(half) == 0, 1.0, 2.0).astype(np.float32)[:, None]
    fwd_cos, fwd_sin = twiddle(length, half, length)
    inv_z = np.block([[full_cos[:half], -full_sin[:half]], [full_sin[:half], full_cos[:half]]])
    inv_y = np.block([[full_cos, -full_sin], [full_sin, full_cos]])
    q, h, c, p, k = np.meshgrid(
        np.arange(sides), np.arange(2), np.arange(rows // CHUNK), np.arange(2), np.arange(CHUNK), indexing="ij"
    )
    inv_y = inv_y[:, ((q + h * sides) * rows + c * CHUNK + k + p * length).reshape(-1)]
    inv_x = np.concatenate([inv_cos * weight, -inv_sin * weight], axis=0)
    order = np.concatenate([(3 - l) * quarter + np.arange(quarter) for l in range(4)])
    fwd_x = np.concatenate([fwd_cos[:, order], -fwd_sin[:, order]], axis=1)
    fwd_y = np.block([[full_cos, full_sin], [-full_sin, full_cos]])
    z, s, p = np.meshgrid(np.arange(rows), np.arange(n), np.arange(2), indexing="ij")
    fwd_z = fwd_y[:, (s * rows + z + p * length).reshape(-1)]
    return tuple(
        jnp.asarray(t.astype(np.float32).astype(jnp.bfloat16)) for t in (inv_z, inv_y, inv_x, fwd_x, fwd_y, fwd_z)
    )


def dot(a, b):
    return jnp.dot(a, b, preferred_element_type=jnp.float32)


def step_kernel(n, m, rows, band, *refs):
    (state, vel, species, ktable, bounds, inv_z_in, inv_y_in, inv_x_in, fwd_x_in, fwd_y_in, fwd_z_in,
     spread, partial, kap,
     inv_z, inv_y, inv_x, base_x, fwd_y, fwd_z, fwd_x, out, lined, tb, wsend, recv, tmp, uall, fsend, raw, packed, tf, zin, iny, inx, peak, acc, stat, stats,
     s_load, tab_load, a_out, l_out, x_send, x_recv, w_send, w_recv, u_send, u_recv, u_loc,
     f_send, f_recv, t_send, t_recv, free) = refs
    length = n * rows
    half = length // 2
    quarter = half // 4
    sides = n // 2
    nch = rows // CHUNK
    groups = rows // 4
    f32 = jnp.float32
    bf16 = jnp.bfloat16
    step_size = cfl_number * 2.0 * math.pi / length
    cells = float(length) ** 3
    me = lax.axis_index("fft")
    mine = lax.axis_index("scal")
    side = me // sides
    place = me % sides
    partner = (me + sides) % n

    def each(low, high, act):
        def one(j, carry):
            act(j)
            return carry

        lax.fori_loop(low, high, one, 0)

    def load_copy(c):
        at = pl.ds(c * CHUNK, CHUNK)
        return pltpu.make_async_copy(state.at[:, at], out.at[:, at], s_load.at[c])

    def swap_copy(c, h):
        at = pl.ds(c * CHUNK, CHUNK)
        return pltpu.make_async_remote_copy(
            src_ref=tb.at[h, at], dst_ref=tb.at[h, at], send_sem=x_send, recv_sem=x_recv.at[c],
            device_id={"fft": partner}, device_id_type=MESH,
        )

    def row_copy(kind, h, c, to, slot):
        at = pl.ds(0, rows) if kind == 0 else pl.ds((kind - 1) * (rows // 2), rows // 2)
        return pltpu.make_async_remote_copy(
            src_ref=wsend.at[h, c, to, at], dst_ref=recv.at[slot, h, c, at],
            send_sem=w_send.at[kind], recv_sem=w_recv.at[kind],
            device_id={"fft": side * sides + to}, device_id_type=MESH,
        )

    def partial_copy(c):
        at = pl.ds(c * CHUNK, CHUNK)
        return pltpu.make_async_copy(out.at[:, at], partial.at[:, at], a_out)

    def spread_copy(i):
        return pltpu.make_async_copy(lined.at[i], spread.at[i], l_out)

    def speed_copy(s, slot):
        return pltpu.make_async_remote_copy(
            src_ref=vel, dst_ref=uall.at[:, :, slot], send_sem=u_send, recv_sem=u_recv,
            device_id={"scal": s}, device_id_type=MESH,
        )

    def own_speed():
        return pltpu.make_async_copy(vel, uall.at[:, :, mine], u_loc)

    def await_bytes(ref, sem):
        pltpu.make_async_copy(ref, ref, sem).wait()

    def forward_copy(st, g, d, h, slot, k):
        return pltpu.make_async_remote_copy(
            src_ref=fsend.at[d % sides + h * sides, g, pl.ds(0, k)], dst_ref=raw.at[h, slot, g, pl.ds(0, k)],
            send_sem=f_send.at[h, d], recv_sem=f_recv.at[st, g, h],
            device_id={"fft": d}, device_id_type=MESH,
        )

    def stat_copy(d, slot):
        return pltpu.make_async_remote_copy(
            src_ref=stat, dst_ref=stats.at[slot], send_sem=t_send, recv_sem=t_recv,
            device_id={"fft": d}, device_id_type=MESH,
        )

    def needed(b, t):
        low = b * rows
        least = jnp.where(low < half, low, length - low - rows + 1)
        return (t * quarter) ** 2 + least * least <= band * band

    def by_tiles(b, act):
        for k in range(1, 4):
            wanted = needed(b, k - 1)
            if k < 3:
                wanted = jnp.logical_and(wanted, jnp.logical_not(needed(b, k)))

            @pl.when(wanted)
            def _():
                act(k)

    def chunk_inside(h, c):
        low = (place + h * sides) * rows + c * CHUNK
        least = jnp.where(low < half, low, length - low - CHUNK + 1)
        return least <= band

    table_copies = [
        pltpu.make_async_copy(a, b, tab_load.at[i]) for i, (a, b) in enumerate([
            (inv_z_in, inv_z), (inv_y_in, inv_y), (inv_x_in, inv_x), (fwd_x_in, base_x), (fwd_y_in, fwd_y),
            (fwd_z_in, fwd_z)])
    ]
    table_copies[0].start()
    each(0, nch, lambda c: load_copy(c).start())
    for copy in table_copies[1:]:
        copy.start()

    barrier = pltpu.get_barrier_semaphore()
    each(1, n, lambda j: pl.semaphore_signal(
        barrier, inc=1, device_id={"fft": (me + j) % n}, device_id_type=MESH))
    each(1, m, lambda j: pl.semaphore_signal(
        barrier, inc=1, device_id={"scal": (mine + j) % m}, device_id_type=MESH))

    lane = lax.broadcasted_iota(jnp.int32, (half, 2 * length), 1) % length
    flip = jnp.where((lane % 2) * side == 1, -1.0, 1.0)
    kz_lane = jnp.where(lane < half, lane, lane - length).astype(f32)
    table_copies[0].wait()
    real_z = inv_z[:half].astype(f32) * flip
    imag_z = inv_z[half:].astype(f32) * flip
    zin[0:half] = real_z.astype(bf16)
    zin[half:length] = imag_z.astype(bf16)
    zin[length:length + half] = (-kz_lane * imag_z).astype(bf16)
    zin[length + half:] = (kz_lane * real_z).astype(bf16)

    pl.semaphore_wait(barrier, n + m - 2)

    def z_pair(pr, pair):
        res = dot(zin[...], pair)
        for k in range(2):
            for f in range(2):
                for p in range(2):
                    at = f * length + p * half
                    tmp[f, pl.ds(p * CHUNK + 2 * pr + k, half, stride=2 * CHUNK), :] = (
                        res[at:at + half, k * half:(k + 1) * half]
                    )

    def send_rows(kind, h, c):
        both = jnp.concatenate([tmp[0].astype(bf16), tmp[1].astype(bf16)], axis=1)
        wsend[h, c] = both.reshape(sides, rows, 2 * CHUNK, 2 * half)
        each(1, sides, lambda j: row_copy(kind, h, c, (place + j) % sides, place).start())
        recv[place, h, c] = wsend[h, c, place]

    def begin(i):
        c = i % nch
        own = i < nch
        h = jnp.where(own, side, 1 - side)

        @pl.when(own)
        def _():
            load_copy(c).wait()

            def cast(r):
                tb[side, r] = out[:, r].astype(bf16)

            each(c * CHUNK, c * CHUNK + CHUNK, cast)
            swap_copy(c, side).start()

        @pl.when(jnp.logical_not(own))
        def _():
            swap_copy(c, 1 - side).wait_recv()

        for pr in range(CHUNK // 2):
            r = c * CHUNK + 2 * pr
            z_pair(pr, jnp.concatenate(
                [tb[h, r].reshape(2 * length, half), tb[h, r + 1].reshape(2 * length, half)], axis=1))
        send_rows(0, h, c)

    each(0, nch, begin)
    each(1, m, lambda j: speed_copy((mine + j) % m, mine).start())
    own_speed().start()

    kx = lax.broadcasted_iota(jnp.int32, (length, half), 1).astype(f32)
    kz_row = lax.broadcasted_iota(jnp.int32, (length, half), 0)
    kz = jnp.where(kz_row < half, kz_row, kz_row - length).astype(f32)
    kxz = kx * kx + kz * kz
    weight = jnp.where(kx == 0.0, 1.0, 2.0)

    def ky_square(b, r):
        index = b * rows + r
        wave = jnp.where(index < half, index, index - length)
        return jnp.full((1, half), wave * wave, jnp.int32).astype(f32)

    acc[...] = jnp.zeros_like(acc)

    def add_row(r):
        real, imag = out[0, r], out[1, r]
        energy = weight * (real * real + imag * imag)
        acc[0] += jnp.sum(energy.reshape(length // 8, 8, half), axis=0)
        acc[1] += jnp.sum((energy * (kxz + ky_square(me, r))).reshape(length // 8, 8, half), axis=0)

    each(0, rows, add_row)

    col = lax.broadcasted_iota(jnp.int32, (length, 2 * length), 1)
    row_ky = ((col // (2 * CHUNK * nch * 2)) + ((col // (2 * CHUNK * nch)) % 2) * sides) * rows
    row_ky = row_ky + ((col // (2 * CHUNK)) % nch) * CHUNK + col % CHUNK
    row_ky = jnp.where(row_ky < half, row_ky, row_ky - length).astype(f32)
    for copy in table_copies[1:]:
        copy.wait()
    iny[:length] = (-row_ky * inv_y[length:].astype(f32)).astype(bf16)
    iny[length:] = (row_ky * inv_y[:length].astype(f32)).astype(bf16)
    for i in range(2):
        turn = base_x[:, i * half:(i + 1) * half].astype(f32)
        for p in range(4):
            fwd_x[p, :, i * half:(i + 1) * half] = (pltpu.roll(turn, p * quarter, 1) if p else turn).astype(bf16)
    kx_row = lax.broadcasted_iota(jnp.int32, (half, length), 0).astype(f32)
    inx[:half] = (kx_row * inv_x[half:].astype(f32)).astype(bf16)
    inx[half:] = (-kx_row * inv_x[:half].astype(f32)).astype(bf16)

    for h in range(2):
        for t in range(3):
            @pl.when(jnp.logical_not(needed(place + h * sides, t)))
            def _():
                def clear(j):
                    raw[h, (me + j) % n, :, t] = jnp.zeros((groups, 2, rows, half), bf16)

                each(1, n, clear)

    peak[...] = jnp.zeros_like(peak)

    each(nch, 2 * nch, begin)

    tile_lane = lax.broadcasted_iota(jnp.int32, (2 * length, half), 1) // quarter

    def pick(choices):
        result = choices[-1]
        for i in range(len(choices) - 2, -1, -1):
            result = jnp.where(tile_lane == i, choices[i], result)
        return result

    def pair_planes(st, z, hh):
        blocks = [recv[:, :, :, z + p].reshape(2 * length, 2 * half) for p in range(2)]
        section = dot(inv_y[...], jnp.concatenate(blocks, axis=1)).astype(bf16)
        turned = dot(iny[...], jnp.concatenate([b[:, :half] for b in blocks], axis=1)).astype(bf16)
        halves = []
        for p in range(2):
            at = 2 * half * p
            sides_of = [
                (section[:, at:at + half], inx),
                (turned[:, half * p:half * (p + 1)], inv_x),
                (section[:, at + half:at + 2 * half], inv_x),
            ]
            total = None
            square = None
            for i, (part, table) in enumerate(sides_of):
                lhs = jnp.concatenate([part[:length], part[length:]], axis=1)
                grad = dot(lhs, table[...])
                u = uall[i, z + p].reshape(length, length).astype(f32)
                total = u * grad if total is None else total + u * grad
                if st == 0:
                    square = grad * grad if square is None else square + grad * grad
            if st == 0:
                peak[...] = jnp.maximum(peak[...], jnp.max(square.reshape(length // 8, 8, length), axis=0))
            flat = dot(total.astype(bf16), fwd_x[2 * hh + p]).astype(bf16)
            halves.append(jnp.concatenate([flat[:, :half], flat[:, half:]], axis=0))
        packed[hh] = dot(fwd_y[...], jnp.concatenate(halves, axis=1))

    def for_blocks(st, d, act):
        if st == 0:
            each(0, 2, act)
        else:
            act(d // sides)

    def leave(st, g):
        def one(j):
            d = (me + j) % n
            for_blocks(st, d, lambda h: by_tiles(
                d % sides + h * sides, lambda k: forward_copy(st, g, d, h, me, k).start()))

        each(1, n, one)

    def rows_of(kind):
        return pl.ds(0, rows) if kind == 0 else pl.ds((kind - 1) * (rows // 2), rows // 2)

    def rows_arrive(kind):
        await_bytes(recv.at[pl.ds(0, sides - 1), :, :, rows_of(kind)], w_recv.at[kind])

    def rows_sent(kind):
        await_bytes(wsend.at[:, :, pl.ds(0, sides - 1), rows_of(kind)], w_send.at[kind])

    def run_group(st, g):
        for hh in range(2):
            pair_planes(st, g * 4 + 2 * hh, hh)
        for t in range(3):
            chosen = [(i + 1 + t) % 4 for i in range(4)]
            tile = pick([packed[p // 2, :, (p % 2) * half:(p % 2 + 1) * half] for p in chosen]).astype(bf16)
            for q in range(2):
                fsend[:, g, t, q] = tile[q * length:(q + 1) * length].reshape(n, rows, half)

    def keep_own(g, h):
        raw[h, me, g] = fsend[place + h * sides, g]

    def group_arrive(st, g, h):
        by_tiles(place + h * sides, lambda k: await_bytes(
            raw.at[h, pl.ds(0, n - 1), g, pl.ds(0, k)], f_recv.at[st, g, h]))

    def forward_sent(st):
        def one(j):
            d = (me + j) % n

            def block(h):
                b = d % sides + h * sides
                by_tiles(b, lambda k: await_bytes(fsend.at[b, :, pl.ds(0, k)], f_send.at[h, d]))

            for_blocks(st, d, block)

        each(1, n, one)

    def unpack(st, h):
        def group(g):
            group_arrive(st, g, h)
            tiles = [raw[h, :, g, t].reshape(2 * length, half).astype(f32) for t in range(3)]
            for p in range(4):
                moved = [
                    pltpu.roll(tiles[t], (2 * t + 1 - p) % 4 * quarter, 1) if (2 * t + 1 - p) % 4 else tiles[t]
                    for t in range(3)
                ]
                at = pl.multiple_of((4 * g + p) * 2 * length, 2 * length)
                tf[pl.ds(at, 2 * length), :] = pick(moved + [jnp.zeros_like(tiles[0])])

        each(0, groups, group)

    def row_pair(r):
        return jnp.concatenate(
            [tf[pl.ds(r + k, 2 * length, stride=rows), :].astype(bf16) for k in range(2)], axis=1)

    rows_arrive(0)

    await_bytes(uall.at[:, :, pl.ds(0, m - 1)], u_recv)
    own_speed().wait()

    def first_group(g):
        run_group(0, g)
        for h in range(2):
            keep_own(g, h)

        @pl.when(g == 0)
        def _():
            leave(0, g)

    each(0, groups, first_group)

    line = lax.broadcasted_iota(jnp.int32, (8, 128), 0)
    largest = jnp.sqrt(jnp.max(peak[...], keepdims=True))
    local_var = jnp.sum(acc[0], keepdims=True) / cells
    local_grad = jnp.sum(acc[1], keepdims=True) / cells
    stat[...] = jnp.where(line == 0, local_var, jnp.where(line == 1, local_grad, largest))
    each(1, n, lambda j: stat_copy((me + j) % n, me).start())
    each(1, groups, lambda g: leave(0, g))
    stats[me] = stat[...]
    rows_sent(0)
    await_bytes(stats.at[pl.ds(0, n - 1)], t_recv)
    summed = jnp.sum(stats[...], axis=0)
    highest = jnp.max(stats[...], axis=0)
    kappa = ktable[species[0]] * highest[2:3, :1] * jnp.sqrt(summed[0:1, :1]) / (summed[1:2, :1] + 1e-06)
    kap[...] = jnp.broadcast_to(kappa, kap.shape)
    bound = jnp.full((1, half), bounds[0], jnp.int32).astype(f32)
    bound = bound * bound
    rate = -kappa * step_size

    def second(h, c, own, inside):
        block = place + h * sides
        for pr in range(CHUNK // 2):
            r = c * CHUNK + 2 * pr
            moved = dot(fwd_z[...], row_pair(r)) if inside else None
            cols = []
            for k in range(2):
                square = kxz + ky_square(block, r + k)
                factor = jnp.exp(rate * square)
                keep = square <= bound
                for p in range(2):
                    value = tb[h, r + k, p].astype(f32)
                    if inside:
                        add = moved[p * length:(p + 1) * length, k * half:(k + 1) * half]
                        add = jnp.where(keep, -step_size * add, 0.0)
                        value = value + add
                    cols.append((factor * value).astype(bf16))
                    if own:
                        start = out[p, r + k]
                        out[p, r + k] = factor * (start + 0.5 * add) if inside else factor * start
            z_pair(pr, jnp.concatenate(
                [jnp.concatenate(cols[:2], axis=0), jnp.concatenate(cols[2:], axis=0)], axis=1))
        send_rows(1, h, c)
        if own:
            partial_copy(c).start()

    def chunks(own, inside):
        h = side if own else 1 - side

        def one(c):
            wanted = chunk_inside(h, c)

            @pl.when(wanted if inside else jnp.logical_not(wanted))
            def _():
                second(h, c, own, inside)

        each(0, nch, one)

    for own in (True, False):
        chunks(own, False)
    for own in (True, False):
        unpack(0, side if own else 1 - side)
        if not own:
            each(1, n, lambda j: pl.semaphore_signal(
                free, inc=1, device_id={"fft": (me + j) % n}, device_id_type=MESH))
        chunks(own, True)
    each(0, 2, lambda h: each(0, nch, lambda c: each(
        1, sides, lambda j: row_copy(2, h, c, (place + j) % sides, place).start())))

    forward_sent(0)
    for part in range(2):
        rows_arrive(1 + part)
        if part == 0:
            pl.semaphore_wait(free, n - 1)

        def last_group(g):
            run_group(1, g)
            leave(1, g)
            keep_own(g, side)

        each(part * (groups // 2), (part + 1) * (groups // 2), last_group)

    unpack(1, side)

    def line_up(i):
        lined[i] = row_pair(2 * i)
        spread_copy(i).start()

    each(0, rows // 2, line_up)

    await_bytes(tb.at[side], x_send)
    await_bytes(uall.at[:, :, pl.ds(0, m - 1)], u_send)
    await_bytes(stats.at[pl.ds(0, n - 1)], t_send)
    rows_sent(1)
    rows_sent(2)
    forward_sent(1)
    await_bytes(out, a_out)
    await_bytes(lined, l_out)


def final_kernel(rows, length, spread, partial, kap, bounds, fwd_z, out, kap_out):
    half = length // 2
    f32 = jnp.float32
    step_size = cfl_number * 2.0 * math.pi / length
    kx = lax.broadcasted_iota(jnp.int32, (length, half), 1).astype(f32)
    kz = lax.broadcasted_iota(jnp.int32, (length, half), 0)
    kz = jnp.where(kz < half, kz, kz - length).astype(f32)
    bound = jnp.full((1, half), bounds[0], jnp.int32).astype(f32)
    moved = dot(fwd_z[...], spread[0])
    for k in range(2):
        ky = lax.axis_index("fft") * rows + pl.program_id(0) * 2 + k
        ky = jnp.where(ky < half, ky, ky - length)
        square = kx * kx + kz * kz + jnp.full((1, half), ky * ky, jnp.int32).astype(f32)
        for p in range(2):
            value = moved[p * length:(p + 1) * length, k * half:(k + 1) * half]
            out[p, k] = partial[p, k] + jnp.where(square <= bound * bound, -0.5 * step_size * value, 0.0)
    kap_out[0] = kap[0, 0]


def body(n, m, scalar_state, velocity, species, kappa_table, dealias_bound):
    rows = scalar_state.shape[2]
    length = scalar_state.shape[3]
    half = length // 2
    sides = n // 2
    nch = rows // CHUNK
    groups = rows // 4
    f32, bf16 = jnp.float32, jnp.bfloat16
    tables = lax.optimization_barrier(build_tables(length, n, rows))
    vmem = pl.BlockSpec(memory_space=pltpu.VMEM)
    smem = pl.BlockSpec(memory_space=pltpu.SMEM)
    hbm = pl.BlockSpec(memory_space=pl.ANY)
    dma = pltpu.SemaphoreType.DMA
    scratch = [pltpu.VMEM(t.shape, bf16) for t in tables] + [
        pltpu.VMEM((4, length, length), bf16),
        pltpu.VMEM((2, rows, length, half), f32),
        pltpu.VMEM((rows // 2, 2 * length, 2 * half), bf16),
        pltpu.VMEM((2, rows, 2, length, half), bf16),
        pltpu.VMEM((2, nch, sides, rows, 2 * CHUNK, 2 * half), bf16),
        pltpu.VMEM((sides, 2, nch, rows, 2 * CHUNK, 2 * half), bf16),
        pltpu.VMEM((2, half * 2 * CHUNK, half), f32),
        pltpu.VMEM((3, rows, m, length // m, length), bf16),
        pltpu.VMEM((n, groups, 3, 2, rows, half), bf16),
        pltpu.VMEM((2, n, groups, 3, 2, rows, half), bf16),
        pltpu.VMEM((2, 2 * length, 2 * half), f32),
        pltpu.VMEM((rows * 2 * length, half), f32),
        pltpu.VMEM((2 * length, 2 * length), bf16),
        pltpu.VMEM((2 * length, 2 * length), bf16),
        pltpu.VMEM((length, length), bf16),
        pltpu.VMEM((8, length), f32),
        pltpu.VMEM((2, 8, half), f32),
        pltpu.VMEM((8, 128), f32),
        pltpu.VMEM((n, 8, 128), f32),
        dma((nch,)), dma((len(tables),)), dma, dma, dma, dma((nch,)), dma((3,)), dma((3,)), dma, dma, dma,
        dma((2, n)), dma((2, groups, 2)), dma, dma,
        pltpu.SemaphoreType.REGULAR,
    ]
    spread, partial, kappa = pl.pallas_call(
        functools.partial(step_kernel, n, m, rows, length // 3),
        out_shape=[
            jax.ShapeDtypeStruct((rows // 2, 2 * length, 2 * half), bf16),
            jax.ShapeDtypeStruct((2, rows, length, half), f32),
            jax.ShapeDtypeStruct((8, 128), f32),
        ],
        in_specs=[hbm, hbm, smem, smem, smem] + [hbm] * 6,
        out_specs=[hbm, hbm, vmem],
        scratch_shapes=scratch,
        compiler_params=pltpu.CompilerParams(
            collective_id=0, has_side_effects=True, vmem_limit_bytes=63 * 1024 * 1024,
        ),
        name="whole_step",
    )(scalar_state[0], velocity, species, kappa_table, dealias_bound, *tables)
    new_state, kappa = pl.pallas_call(
        functools.partial(final_kernel, rows, length),
        grid=(rows // 2,),
        out_shape=[
            jax.ShapeDtypeStruct((2, rows, length, half), f32),
            jax.ShapeDtypeStruct((1,), f32),
        ],
        in_specs=[
            pl.BlockSpec((1, 2 * length, 2 * half), lambda i: (i, 0, 0)),
            pl.BlockSpec((2, 2, length, half), lambda i: (0, i, 0, 0)),
            smem, smem, vmem,
        ],
        out_specs=[pl.BlockSpec((2, 2, length, half), lambda i: (0, i, 0, 0)), smem],
        name="final_step",
    )(spread, partial, kappa, dealias_bound, tables[5])
    return new_state[None], kappa


def solution(mesh):
    placed = (
        P("scal", None, "fft", None, None),
        P(None, "fft", "scal", None),
        P("scal"),
        P(),
        P("scal"),
    )
    return jax.shard_map(
        functools.partial(body, mesh.shape["fft"], mesh.shape["scal"]),
        mesh=mesh,
        in_specs=placed,
        out_specs=(P("scal", None, "fft", None, None), P("scal")),
        check_vma=False,
    )
```

```python
import functools
import math

import numpy as np

import jax
import jax.numpy as jnp
from jax import lax
from jax.experimental import pallas as pl
from jax.experimental.pallas import tpu as pltpu
from jax.sharding import PartitionSpec as P

MESH = pl.DeviceIdType.MESH
cfl_number = 0.2
CHUNK = 4


def twiddle(size_in, size_out, length):
    row_index = np.arange(size_in, dtype=np.int32)[:, None]
    col_index = np.arange(size_out, dtype=np.int32)[None, :]
    angles = (row_index * col_index % length).astype(np.float32) * np.float32(2.0 * math.pi / length)
    norming = np.float32(1.0 / math.sqrt(length))
    return (np.cos(angles) * norming, np.sin(angles) * norming)


def build_tables(length, n, rows):
    half = length // 2
    quarter = half // 4
    sides = n // 2
    full_cos, full_sin = twiddle(length, length, length)
    inv_cos, inv_sin = twiddle(half, length, length)
    weight = np.where(np.arange(half) == 0, 1.0, 2.0).astype(np.float32)[:, None]
    fwd_cos, fwd_sin = twiddle(length, half, length)
    inv_z = np.block([[full_cos[:half], -full_sin[:half]], [full_sin[:half], full_cos[:half]]])
    inv_y = np.block([[full_cos, -full_sin], [full_sin, full_cos]])
    q, h, c, p, k = np.meshgrid(
        np.arange(sides), np.arange(2), np.arange(rows // CHUNK), np.arange(2), np.arange(CHUNK), indexing="ij"
    )
    inv_y = inv_y[:, ((q + h * sides) * rows + c * CHUNK + k + p * length).reshape(-1)]
    inv_x = np.concatenate([inv_cos * weight, -inv_sin * weight], axis=0)
    order = np.concatenate([(3 - l) * quarter + np.arange(quarter) for l in range(4)])
    fwd_x = np.concatenate([fwd_cos[:, order], -fwd_sin[:, order]], axis=1)
    fwd_y = np.block([[full_cos, full_sin], [-full_sin, full_cos]])
    z, s, p = np.meshgrid(np.arange(rows), np.arange(n), np.arange(2), indexing="ij")
    fwd_z = fwd_y[:, (s * rows + z + p * length).reshape(-1)]
    return tuple(
        jnp.asarray(t.astype(np.float32).astype(jnp.bfloat16)) for t in (inv_z, inv_y, inv_x, fwd_x, fwd_y, fwd_z)
    )


def dot(a, b):
    return jnp.dot(a, b, preferred_element_type=jnp.float32)


def step_kernel(n, m, rows, band, *refs):
    (state, vel, species, ktable, bounds, inv_z_in, inv_y_in, inv_x_in, fwd_x_in, fwd_y_in, fwd_z_in,
     spread, partial, kap,
     inv_z, inv_y, inv_x, base_x, fwd_y, fwd_z, fwd_x, out, lined, tb, wsend, recv, tmp, uall, fsend, raw, packed, tf, zin, iny, inx, peak, acc, stat, stats,
     s_load, tab_load, a_out, l_out, x_send, x_recv, w_send, w_recv, u_send, u_recv, u_loc,
     f_send, f_recv, t_send, t_recv, free) = refs
    length = n * rows
    half = length // 2
    quarter = half // 4
    sides = n // 2
    nch = rows // CHUNK
    groups = rows // 4
    f32 = jnp.float32
    bf16 = jnp.bfloat16
    step_size = cfl_number * 2.0 * math.pi / length
    cells = float(length) ** 3
    me = lax.axis_index("fft")
    mine = lax.axis_index("scal")
    side = me // sides
    place = me % sides
    partner = (me + sides) % n

    def each(low, high, act):
        def one(j, carry):
            act(j)
            return carry

        lax.fori_loop(low, high, one, 0)

    def load_copy(c):
        at = pl.ds(c * CHUNK, CHUNK)
        return pltpu.make_async_copy(state.at[:, at], out.at[:, at], s_load.at[c])

    def swap_copy(c, h):
        at = pl.ds(c * CHUNK, CHUNK)
        return pltpu.make_async_remote_copy(
            src_ref=tb.at[h, at], dst_ref=tb.at[h, at], send_sem=x_send, recv_sem=x_recv.at[c],
            device_id={"fft": partner}, device_id_type=MESH,
        )

    def row_copy(kind, h, c, to, slot):
        at = pl.ds(0, rows) if kind == 0 else pl.ds((kind - 1) * (rows // 2), rows // 2)
        return pltpu.make_async_remote_copy(
            src_ref=wsend.at[h, c, to, at], dst_ref=recv.at[slot, h, c, at],
            send_sem=w_send.at[kind], recv_sem=w_recv.at[kind],
            device_id={"fft": side * sides + to}, device_id_type=MESH,
        )

    def partial_copy(c):
        at = pl.ds(c * CHUNK, CHUNK)
        return pltpu.make_async_copy(out.at[:, at], partial.at[:, at], a_out)

    def spread_copy(i):
        return pltpu.make_async_copy(lined.at[i], spread.at[i], l_out)

    def speed_copy(s, slot):
        return pltpu.make_async_remote_copy(
            src_ref=vel, dst_ref=uall.at[:, :, slot], send_sem=u_send, recv_sem=u_recv,
            device_id={"scal": s}, device_id_type=MESH,
        )

    def own_speed():
        return pltpu.make_async_copy(vel, uall.at[:, :, mine], u_loc)

    def await_bytes(ref, sem):
        pltpu.make_async_copy(ref, ref, sem).wait()

    def forward_copy(st, g, d, h, slot, k):
        return pltpu.make_async_remote_copy(
            src_ref=fsend.at[d % sides + h * sides, g, pl.ds(0, k)], dst_ref=raw.at[h, slot, g, pl.ds(0, k)],
            send_sem=f_send.at[h, d], recv_sem=f_recv.at[st, g, h],
            device_id={"fft": d}, device_id_type=MESH,
        )

    def stat_copy(d, slot):
        return pltpu.make_async_remote_copy(
            src_ref=stat, dst_ref=stats.at[slot], send_sem=t_send, recv_sem=t_recv,
            device_id={"fft": d}, device_id_type=MESH,
        )

    def needed(b, t):
        low = b * rows
        least = jnp.where(low < half, low, length - low - rows + 1)
        return (t * quarter) ** 2 + least * least <= band * band

    def by_tiles(b, act):
        for k in range(1, 4):
            wanted = needed(b, k - 1)
            if k < 3:
                wanted = jnp.logical_and(wanted, jnp.logical_not(needed(b, k)))

            @pl.when(wanted)
            def _():
                act(k)

    def chunk_inside(h, c):
        low = (place + h * sides) * rows + c * CHUNK
        least = jnp.where(low < half, low, length - low - CHUNK + 1)
        return least <= band

    table_copies = [
        pltpu.make_async_copy(a, b, tab_load.at[i]) for i, (a, b) in enumerate([
            (inv_z_in, inv_z), (inv_y_in, inv_y), (inv_x_in, inv_x), (fwd_x_in, base_x), (fwd_y_in, fwd_y),
            (fwd_z_in, fwd_z)])
    ]
    table_copies[0].start()
    each(0, nch, lambda c: load_copy(c).start())
    for copy in table_copies[1:]:
        copy.start()

    barrier = pltpu.get_barrier_semaphore()
    each(1, n, lambda j: pl.semaphore_signal(
        barrier, inc=1, device_id={"fft": (me + j) % n}, device_id_type=MESH))
    each(1, m, lambda j: pl.semaphore_signal(
        barrier, inc=1, device_id={"scal": (mine + j) % m}, device_id_type=MESH))

    lane = lax.broadcasted_iota(jnp.int32, (half, 2 * length), 1) % length
    flip = jnp.where((lane % 2) * side == 1, -1.0, 1.0)
    kz_lane = jnp.where(lane < half, lane, lane - length).astype(f32)
    table_copies[0].wait()
    real_z = inv_z[:half].astype(f32) * flip
    imag_z = inv_z[half:].astype(f32) * flip
    zin[0:half] = real_z.astype(bf16)
    zin[half:length] = imag_z.astype(bf16)
    zin[length:length + half] = (-kz_lane * imag_z).astype(bf16)
    zin[length + half:] = (kz_lane * real_z).astype(bf16)

    pl.semaphore_wait(barrier, n + m - 2)

    def z_pair(pr, pair):
        res = dot(zin[...], pair)
        for k in range(2):
            for f in range(2):
                for p in range(2):
                    at = f * length + p * half
                    tmp[f, pl.ds(p * CHUNK + 2 * pr + k, half, stride=2 * CHUNK), :] = (
                        res[at:at + half, k * half:(k + 1) * half]
                    )

    def send_rows(kind, h, c):
        both = jnp.concatenate([tmp[0].astype(bf16), tmp[1].astype(bf16)], axis=1)
        wsend[h, c] = both.reshape(sides, rows, 2 * CHUNK, 2 * half)
        each(1, sides, lambda j: row_copy(kind, h, c, (place + j) % sides, place).start())
        recv[place, h, c] = wsend[h, c, place]

    def begin(i):
        c = i % nch
        own = i < nch
        h = jnp.where(own, side, 1 - side)

        @pl.when(own)
        def _():
            load_copy(c).wait()

            def cast(r):
                tb[side, r] = out[:, r].astype(bf16)

            each(c * CHUNK, c * CHUNK + CHUNK, cast)
            swap_copy(c, side).start()

        @pl.when(jnp.logical_not(own))
        def _():
            swap_copy(c, 1 - side).wait_recv()

        for pr in range(CHUNK // 2):
            r = c * CHUNK + 2 * pr
            z_pair(pr, jnp.concatenate(
                [tb[h, r].reshape(2 * length, half), tb[h, r + 1].reshape(2 * length, half)], axis=1))
        send_rows(0, h, c)

    each(0, nch, begin)
    each(1, m, lambda j: speed_copy((mine + j) % m, mine).start())
    own_speed().start()

    kx = lax.broadcasted_iota(jnp.int32, (length, half), 1).astype(f32)
    kz_row = lax.broadcasted_iota(jnp.int32, (length, half), 0)
    kz = jnp.where(kz_row < half, kz_row, kz_row - length).astype(f32)
    kxz = kx * kx + kz * kz
    weight = jnp.where(kx == 0.0, 1.0, 2.0)

    def ky_square(b, r):
        index = b * rows + r
        wave = jnp.where(index < half, index, index - length)
        return jnp.full((1, half), wave * wave, jnp.int32).astype(f32)

    acc[...] = jnp.zeros_like(acc)

    def add_row(r):
        real, imag = out[0, r], out[1, r]
        energy = weight * (real * real + imag * imag)
        acc[0] += jnp.sum(energy.reshape(length // 8, 8, half), axis=0)
        acc[1] += jnp.sum((energy * (kxz + ky_square(me, r))).reshape(length // 8, 8, half), axis=0)

    each(0, rows, add_row)

    col = lax.broadcasted_iota(jnp.int32, (length, 2 * length), 1)
    row_ky = ((col // (2 * CHUNK * nch * 2)) + ((col // (2 * CHUNK * nch)) % 2) * sides) * rows
    row_ky = row_ky + ((col // (2 * CHUNK)) % nch) * CHUNK + col % CHUNK
    row_ky = jnp.where(row_ky < half, row_ky, row_ky - length).astype(f32)
    for copy in table_copies[1:]:
        copy.wait()
    iny[:length] = (-row_ky * inv_y[length:].astype(f32)).astype(bf16)
    iny[length:] = (row_ky * inv_y[:length].astype(f32)).astype(bf16)
    for i in range(2):
        turn = base_x[:, i * half:(i + 1) * half].astype(f32)
        for p in range(4):
            fwd_x[p, :, i * half:(i + 1) * half] = (pltpu.roll(turn, p * quarter, 1) if p else turn).astype(bf16)
    kx_row = lax.broadcasted_iota(jnp.int32, (half, length), 0).astype(f32)
    inx[:half] = (kx_row * inv_x[half:].astype(f32)).astype(bf16)
    inx[half:] = (-kx_row * inv_x[:half].astype(f32)).astype(bf16)

    for h in range(2):
        for t in range(3):
            @pl.when(jnp.logical_not(needed(place + h * sides, t)))
            def _():
                def clear(j):
                    raw[h, (me + j) % n, :, t] = jnp.zeros((groups, 2, rows, half), bf16)

                each(1, n, clear)

    peak[...] = jnp.zeros_like(peak)

    each(nch, 2 * nch, begin)

    tile_lane = lax.broadcasted_iota(jnp.int32, (2 * length, half), 1) // quarter

    def pick(choices):
        result = choices[-1]
        for i in range(len(choices) - 2, -1, -1):
            result = jnp.where(tile_lane == i, choices[i], result)
        return result

    def pair_planes(st, z, hh):
        blocks = [recv[:, :, :, z + p].reshape(2 * length, 2 * half) for p in range(2)]
        section = dot(inv_y[...], jnp.concatenate(blocks, axis=1)).astype(bf16)
        turned = dot(iny[...], jnp.concatenate([b[:, :half] for b in blocks], axis=1)).astype(bf16)
        halves = []
        for p in range(2):
            at = 2 * half * p
            sides_of = [
                (section[:, at:at + half], inx),
                (turned[:, half * p:half * (p + 1)], inv_x),
                (section[:, at + half:at + 2 * half], inv_x),
            ]
            total = None
            square = None
            for i, (part, table) in enumerate(sides_of):
                lhs = jnp.concatenate([part[:length], part[length:]], axis=1)
                grad = dot(lhs, table[...])
                u = uall[i, z + p].reshape(length, length).astype(f32)
                total = u * grad if total is None else total + u * grad
                if st == 0:
                    square = grad * grad if square is None else square + grad * grad
            if st == 0:
                peak[...] = jnp.maximum(peak[...], jnp.max(square.reshape(length // 8, 8, length), axis=0))
            flat = dot(total.astype(bf16), fwd_x[2 * hh + p]).astype(bf16)
            halves.append(jnp.concatenate([flat[:, :half], flat[:, half:]], axis=0))
        packed[hh] = dot(fwd_y[...], jnp.concatenate(halves, axis=1))

    def for_blocks(st, d, act):
        if st == 0:
            each(0, 2, act)
        else:
            act(d // sides)

    def leave(st, low, high, own):
        def one(j):
            d = (me + j) % n
            h = d // sides if own else 1 - d // sides
            by_tiles(d % sides + h * sides, lambda k: each(
                low, high, lambda g: forward_copy(st, g, d, h, me, k).start()))

        each(1, n, one)

    def rows_of(kind):
        return pl.ds(0, rows) if kind == 0 else pl.ds((kind - 1) * (rows // 2), rows // 2)

    def rows_arrive(kind):
        await_bytes(recv.at[pl.ds(0, sides - 1), :, :, rows_of(kind)], w_recv.at[kind])

    def rows_sent(kind):
        await_bytes(wsend.at[:, :, pl.ds(0, sides - 1), rows_of(kind)], w_send.at[kind])

    def run_group(st, g):
        for hh in range(2):
            pair_planes(st, g * 4 + 2 * hh, hh)
        for t in range(3):
            chosen = [(i + 1 + t) % 4 for i in range(4)]
            tile = pick([packed[p // 2, :, (p % 2) * half:(p % 2 + 1) * half] for p in chosen]).astype(bf16)
            for q in range(2):
                fsend[:, g, t, q] = tile[q * length:(q + 1) * length].reshape(n, rows, half)

    def keep_own(g, h):
        raw[h, me, g] = fsend[place + h * sides, g]

    def group_arrive(st, g, h):
        by_tiles(place + h * sides, lambda k: await_bytes(
            raw.at[h, pl.ds(0, n - 1), g, pl.ds(0, k)], f_recv.at[st, g, h]))

    def forward_sent(st):
        def one(j):
            d = (me + j) % n

            def block(h):
                b = d % sides + h * sides
                by_tiles(b, lambda k: await_bytes(fsend.at[b, :, pl.ds(0, k)], f_send.at[h, d]))

            for_blocks(st, d, block)

        each(1, n, one)

    def unpack(st, h):
        def group(g):
            group_arrive(st, g, h)
            tiles = [raw[h, :, g, t].reshape(2 * length, half).astype(f32) for t in range(3)]
            for p in range(4):
                moved = [
                    pltpu.roll(tiles[t], (2 * t + 1 - p) % 4 * quarter, 1) if (2 * t + 1 - p) % 4 else tiles[t]
                    for t in range(3)
                ]
                at = pl.multiple_of((4 * g + p) * 2 * length, 2 * length)
                tf[pl.ds(at, 2 * length), :] = pick(moved + [jnp.zeros_like(tiles[0])])

        each(0, groups, group)

    def row_pair(r):
        return jnp.concatenate(
            [tf[pl.ds(r + k, 2 * length, stride=rows), :].astype(bf16) for k in range(2)], axis=1)

    rows_arrive(0)

    await_bytes(uall.at[:, :, pl.ds(0, m - 1)], u_recv)
    own_speed().wait()

    def first_group(g):
        run_group(0, g)
        for h in range(2):
            keep_own(g, h)

        @pl.when(g < 2)
        def _():
            leave(0, g, g + 1, True)

    each(0, groups, first_group)

    line = lax.broadcasted_iota(jnp.int32, (8, 128), 0)
    largest = jnp.sqrt(jnp.max(peak[...], keepdims=True))
    local_var = jnp.sum(acc[0], keepdims=True) / cells
    local_grad = jnp.sum(acc[1], keepdims=True) / cells
    stat[...] = jnp.where(line == 0, local_var, jnp.where(line == 1, local_grad, largest))
    each(1, n, lambda j: stat_copy((me + j) % n, me).start())
    leave(0, 2, groups, True)
    leave(0, 0, groups, False)
    stats[me] = stat[...]
    rows_sent(0)
    await_bytes(stats.at[pl.ds(0, n - 1)], t_recv)
    summed = jnp.sum(stats[...], axis=0)
    highest = jnp.max(stats[...], axis=0)
    kappa = ktable[species[0]] * highest[2:3, :1] * jnp.sqrt(summed[0:1, :1]) / (summed[1:2, :1] + 1e-06)
    kap[...] = jnp.broadcast_to(kappa, kap.shape)
    bound = jnp.full((1, half), bounds[0], jnp.int32).astype(f32)
    bound = bound * bound
    rate = -kappa * step_size

    def send_upper(h, c):
        each(1, sides, lambda j: row_copy(2, h, c, (place + j) % sides, place).start())

    def second(h, c, own, inside):
        block = place + h * sides
        for pr in range(CHUNK // 2):
            r = c * CHUNK + 2 * pr
            moved = dot(fwd_z[...], row_pair(r)) if inside else None
            cols = []
            for k in range(2):
                square = kxz + ky_square(block, r + k)
                factor = jnp.exp(rate * square)
                keep = square <= bound
                for p in range(2):
                    value = tb[h, r + k, p].astype(f32)
                    if inside:
                        add = moved[p * length:(p + 1) * length, k * half:(k + 1) * half]
                        add = jnp.where(keep, -step_size * add, 0.0)
                        value = value + add
                    cols.append((factor * value).astype(bf16))
                    if own:
                        start = out[p, r + k]
                        out[p, r + k] = factor * (start + 0.5 * add) if inside else factor * start
            z_pair(pr, jnp.concatenate(
                [jnp.concatenate(cols[:2], axis=0), jnp.concatenate(cols[2:], axis=0)], axis=1))
        send_rows(1, h, c)
        if not inside:
            send_upper(h, c)
        if own:
            partial_copy(c).start()

    def chunks(own, inside):
        h = side if own else 1 - side

        def one(c):
            wanted = chunk_inside(h, c)

            @pl.when(wanted if inside else jnp.logical_not(wanted))
            def _():
                second(h, c, own, inside)

        each(0, nch, one)

    for own in (True, False):
        chunks(own, False)
    for own in (True, False):
        unpack(0, side if own else 1 - side)
        if not own:
            each(1, n, lambda j: pl.semaphore_signal(
                free, inc=1, device_id={"fft": (me + j) % n}, device_id_type=MESH))
        chunks(own, True)

    def upper(i):
        h, c = i // nch, i % nch

        @pl.when(chunk_inside(h, c))
        def _():
            send_upper(h, c)

    each(0, 2 * nch, upper)

    forward_sent(0)
    for part in range(2):
        rows_arrive(1 + part)
        if part == 0:
            pl.semaphore_wait(free, n - 1)

        def last_group(g):
            run_group(1, g)
            leave(1, g, g + 1, True)
            keep_own(g, side)

        each(part * (groups // 2), (part + 1) * (groups // 2), last_group)

    unpack(1, side)

    def line_up(i):
        lined[i] = row_pair(2 * i)
        spread_copy(i).start()

    each(0, rows // 2, line_up)

    await_bytes(tb.at[side], x_send)
    await_bytes(uall.at[:, :, pl.ds(0, m - 1)], u_send)
    await_bytes(stats.at[pl.ds(0, n - 1)], t_send)
    rows_sent(1)
    rows_sent(2)
    forward_sent(1)
    await_bytes(out, a_out)
    await_bytes(lined, l_out)


def final_kernel(rows, length, spread, partial, kap, bounds, fwd_z_in, out, kap_out, fwd_z, lined, base, done,
                 t_load, l_load, b_load, d_out):
    half = length // 2
    f32 = jnp.float32
    step_size = cfl_number * 2.0 * math.pi / length
    pairs = rows // 2

    def each(act):
        def one(i, carry):
            act(i)
            return carry

        lax.fori_loop(0, pairs, one, 0)

    def line_copy(i):
        return pltpu.make_async_copy(spread.at[i], lined.at[i], l_load.at[i])

    def base_copy(i):
        at = pl.ds(2 * i, 2)
        return pltpu.make_async_copy(partial.at[:, at], base.at[:, at], b_load.at[i])

    def done_copy(i):
        at = pl.ds(2 * i, 2)
        return pltpu.make_async_copy(done.at[:, at], out.at[:, at], d_out.at[i])

    table = pltpu.make_async_copy(fwd_z_in, fwd_z, t_load)
    table.start()

    def load(i):
        line_copy(i).start()
        base_copy(i).start()

    each(load)
    kx = lax.broadcasted_iota(jnp.int32, (length, half), 1).astype(f32)
    kz = lax.broadcasted_iota(jnp.int32, (length, half), 0)
    kz = jnp.where(kz < half, kz, kz - length).astype(f32)
    bound = jnp.full((1, half), bounds[0], jnp.int32).astype(f32)
    kxz = kx * kx + kz * kz
    kap_out[0] = kap[0, 0]
    table.wait()

    def pair(i):
        line_copy(i).wait()
        base_copy(i).wait()
        moved = dot(fwd_z[...], lined[i])
        for k in range(2):
            ky = lax.axis_index("fft") * rows + i * 2 + k
            ky = jnp.where(ky < half, ky, ky - length)
            keep = kxz + jnp.full((1, half), ky * ky, jnp.int32).astype(f32) <= bound * bound
            for p in range(2):
                value = moved[p * length:(p + 1) * length, k * half:(k + 1) * half]
                done[p, 2 * i + k] = base[p, 2 * i + k] + jnp.where(keep, -0.5 * step_size * value, 0.0)
        done_copy(i).start()

    each(pair)
    each(lambda i: done_copy(i).wait())


def body(n, m, scalar_state, velocity, species, kappa_table, dealias_bound):
    rows = scalar_state.shape[2]
    length = scalar_state.shape[3]
    half = length // 2
    sides = n // 2
    nch = rows // CHUNK
    groups = rows // 4
    f32, bf16 = jnp.float32, jnp.bfloat16
    tables = lax.optimization_barrier(build_tables(length, n, rows))
    vmem = pl.BlockSpec(memory_space=pltpu.VMEM)
    smem = pl.BlockSpec(memory_space=pltpu.SMEM)
    hbm = pl.BlockSpec(memory_space=pl.ANY)
    dma = pltpu.SemaphoreType.DMA
    scratch = [pltpu.VMEM(t.shape, bf16) for t in tables] + [
        pltpu.VMEM((4, length, length), bf16),
        pltpu.VMEM((2, rows, length, half), f32),
        pltpu.VMEM((rows // 2, 2 * length, 2 * half), bf16),
        pltpu.VMEM((2, rows, 2, length, half), bf16),
        pltpu.VMEM((2, nch, sides, rows, 2 * CHUNK, 2 * half), bf16),
        pltpu.VMEM((sides, 2, nch, rows, 2 * CHUNK, 2 * half), bf16),
        pltpu.VMEM((2, half * 2 * CHUNK, half), f32),
        pltpu.VMEM((3, rows, m, length // m, length), bf16),
        pltpu.VMEM((n, groups, 3, 2, rows, half), bf16),
        pltpu.VMEM((2, n, groups, 3, 2, rows, half), bf16),
        pltpu.VMEM((2, 2 * length, 2 * half), f32),
        pltpu.VMEM((rows * 2 * length, half), f32),
        pltpu.VMEM((2 * length, 2 * length), bf16),
        pltpu.VMEM((2 * length, 2 * length), bf16),
        pltpu.VMEM((length, length), bf16),
        pltpu.VMEM((8, length), f32),
        pltpu.VMEM((2, 8, half), f32),
        pltpu.VMEM((8, 128), f32),
        pltpu.VMEM((n, 8, 128), f32),
        dma((nch,)), dma((len(tables),)), dma, dma, dma, dma((nch,)), dma((3,)), dma((3,)), dma, dma, dma,
        dma((2, n)), dma((2, groups, 2)), dma, dma,
        pltpu.SemaphoreType.REGULAR,
    ]
    spread, partial, kappa = pl.pallas_call(
        functools.partial(step_kernel, n, m, rows, length // 3),
        out_shape=[
            jax.ShapeDtypeStruct((rows // 2, 2 * length, 2 * half), bf16),
            jax.ShapeDtypeStruct((2, rows, length, half), f32),
            jax.ShapeDtypeStruct((8, 128), f32),
        ],
        in_specs=[hbm, hbm, smem, smem, smem] + [hbm] * 6,
        out_specs=[hbm, hbm, vmem],
        scratch_shapes=scratch,
        compiler_params=pltpu.CompilerParams(
            collective_id=0, has_side_effects=True, vmem_limit_bytes=63 * 1024 * 1024,
        ),
        name="whole_step",
    )(scalar_state[0], velocity, species, kappa_table, dealias_bound, *tables)
    new_state, kappa = pl.pallas_call(
        functools.partial(final_kernel, rows, length),
        out_shape=[
            jax.ShapeDtypeStruct((2, rows, length, half), f32),
            jax.ShapeDtypeStruct((1,), f32),
        ],
        in_specs=[hbm, hbm, smem, smem, hbm],
        out_specs=[hbm, smem],
        scratch_shapes=[
            pltpu.VMEM((2 * length, 2 * length), bf16),
            pltpu.VMEM((rows // 2, 2 * length, 2 * half), bf16),
            pltpu.VMEM((2, rows, length, half), f32),
            pltpu.VMEM((2, rows, length, half), f32),
            dma, dma((rows // 2,)), dma((rows // 2,)), dma((rows // 2,)),
        ],
        name="final_step",
    )(spread, partial, kappa, dealias_bound, tables[5])
    return new_state[None], kappa


def solution(mesh):
    placed = (
        P("scal", None, "fft", None, None),
        P(None, "fft", "scal", None),
        P("scal"),
        P(),
        P("scal"),
    )
    return jax.shard_map(
        functools.partial(body, mesh.shape["fft"], mesh.shape["scal"]),
        mesh=mesh,
        in_specs=placed,
        out_specs=(P("scal", None, "fft", None, None), P("scal")),
        check_vma=False,
    )
```

```python
import functools
import math

import numpy as np

import jax
import jax.numpy as jnp
from jax import lax
from jax.experimental import pallas as pl
from jax.experimental.pallas import tpu as pltpu
from jax.sharding import PartitionSpec as P

MESH = pl.DeviceIdType.MESH
cfl_number = 0.2
CHUNK = 4


def twiddle(size_in, size_out, length):
    row_index = np.arange(size_in, dtype=np.int32)[:, None]
    col_index = np.arange(size_out, dtype=np.int32)[None, :]
    angles = (row_index * col_index % length).astype(np.float32) * np.float32(2.0 * math.pi / length)
    norming = np.float32(1.0 / math.sqrt(length))
    return (np.cos(angles) * norming, np.sin(angles) * norming)


def build_tables(length, n, rows):
    half = length // 2
    quarter = half // 4
    sides = n // 2
    full_cos, full_sin = twiddle(length, length, length)
    inv_cos, inv_sin = twiddle(half, length, length)
    weight = np.where(np.arange(half) == 0, 1.0, 2.0).astype(np.float32)[:, None]
    fwd_cos, fwd_sin = twiddle(length, half, length)
    inv_z = np.block([[full_cos[:half], -full_sin[:half]], [full_sin[:half], full_cos[:half]]])
    inv_y = np.block([[full_cos, -full_sin], [full_sin, full_cos]])
    q, h, c, p, k = np.meshgrid(
        np.arange(sides), np.arange(2), np.arange(rows // CHUNK), np.arange(2), np.arange(CHUNK), indexing="ij"
    )
    inv_y = inv_y[:, ((q + h * sides) * rows + c * CHUNK + k + p * length).reshape(-1)]
    inv_x = np.concatenate([inv_cos * weight, -inv_sin * weight], axis=0)
    order = np.concatenate([(3 - l) * quarter + np.arange(quarter) for l in range(4)])
    fwd_x = np.concatenate([fwd_cos[:, order], -fwd_sin[:, order]], axis=1)
    fwd_y = np.block([[full_cos, full_sin], [-full_sin, full_cos]])
    z, s, p = np.meshgrid(np.arange(rows), np.arange(n), np.arange(2), indexing="ij")
    fwd_z = fwd_y[:, (s * rows + z + p * length).reshape(-1)]
    return tuple(
        jnp.asarray(t.astype(np.float32).astype(jnp.bfloat16)) for t in (inv_z, inv_y, inv_x, fwd_x, fwd_y, fwd_z)
    )


def dot(a, b):
    return jnp.dot(a, b, preferred_element_type=jnp.float32)


def step_kernel(n, m, rows, band, *refs):
    (state, vel, species, ktable, bounds, inv_z_in, inv_y_in, inv_x_in, fwd_x_in, fwd_y_in, fwd_z_in,
     out, lined, kap,
     inv_z, inv_y, inv_x, base_x, fwd_y, fwd_z, fwd_x, tb, wsend, recv, tmp, uall, fsend, raw, packed, tf, zin, iny, inx, peak, acc, stat, stats,
     s_load, tab_load, x_send, x_recv, w_send, w_recv, u_send, u_recv, u_loc,
     f_send, f_recv, t_send, t_recv, free) = refs
    length = n * rows
    half = length // 2
    quarter = half // 4
    sides = n // 2
    nch = rows // CHUNK
    groups = rows // 4
    f32 = jnp.float32
    bf16 = jnp.bfloat16
    step_size = cfl_number * 2.0 * math.pi / length
    cells = float(length) ** 3
    me = lax.axis_index("fft")
    mine = lax.axis_index("scal")
    side = me // sides
    place = me % sides
    partner = (me + sides) % n

    def each(low, high, act):
        def one(j, carry):
            act(j)
            return carry

        lax.fori_loop(low, high, one, 0)

    def load_copy(c):
        at = pl.ds(c * CHUNK, CHUNK)
        return pltpu.make_async_copy(state.at[:, at], out.at[:, at], s_load.at[c])

    def swap_copy(c, h):
        at = pl.ds(c * CHUNK, CHUNK)
        return pltpu.make_async_remote_copy(
            src_ref=tb.at[h, at], dst_ref=tb.at[h, at], send_sem=x_send, recv_sem=x_recv.at[c],
            device_id={"fft": partner}, device_id_type=MESH,
        )

    lower = groups // 2

    def planes_of(kind):
        if isinstance(kind, int) and kind in (0, 2):
            return pl.ds(0, lower * 4)
        if isinstance(kind, int) and kind == 1:
            return pl.ds(lower * 4, (groups - lower) * 4)
        return pl.ds((lower + kind - 3) * 4, 4)

    uppers = range(3, 3 + groups - lower)

    def row_copy(kind, h, c, to, slot):
        at = planes_of(kind)
        return pltpu.make_async_remote_copy(
            src_ref=wsend.at[h, c, to, at], dst_ref=recv.at[slot, h, c, at],
            send_sem=w_send.at[kind], recv_sem=w_recv.at[kind],
            device_id={"fft": side * sides + to}, device_id_type=MESH,
        )

    def block_copy(kind, h, to, slot):
        at = planes_of(kind)
        return pltpu.make_async_remote_copy(
            src_ref=wsend.at[h, :, to, at], dst_ref=recv.at[slot, h, :, at],
            send_sem=w_send.at[kind], recv_sem=w_recv.at[kind],
            device_id={"fft": side * sides + to}, device_id_type=MESH,
        )

    def speed_copy(s, slot):
        return pltpu.make_async_remote_copy(
            src_ref=vel, dst_ref=uall.at[:, :, slot], send_sem=u_send, recv_sem=u_recv,
            device_id={"scal": s}, device_id_type=MESH,
        )

    def own_speed():
        return pltpu.make_async_copy(vel, uall.at[:, :, mine], u_loc)

    def await_bytes(ref, sem):
        pltpu.make_async_copy(ref, ref, sem).wait()

    def forward_copy(st, g, d, h, slot, k):
        return pltpu.make_async_remote_copy(
            src_ref=fsend.at[d % sides + h * sides, g, pl.ds(0, k)], dst_ref=raw.at[h, slot, g, pl.ds(0, k)],
            send_sem=f_send.at[h, d], recv_sem=f_recv.at[st, g, h],
            device_id={"fft": d}, device_id_type=MESH,
        )

    def stat_copy(d, slot):
        return pltpu.make_async_remote_copy(
            src_ref=stat, dst_ref=stats.at[slot], send_sem=t_send, recv_sem=t_recv,
            device_id={"fft": d}, device_id_type=MESH,
        )

    def needed(b, t):
        low = b * rows
        least = jnp.where(low < half, low, length - low - rows + 1)
        return (t * quarter) ** 2 + least * least <= band * band

    def by_tiles(b, act):
        for k in range(1, 4):
            wanted = needed(b, k - 1)
            if k < 3:
                wanted = jnp.logical_and(wanted, jnp.logical_not(needed(b, k)))

            @pl.when(wanted)
            def _():
                act(k)

    def block_inside(h):
        low = (place + h * sides) * rows
        least = jnp.where(low < half, low, length - low - rows + 1)
        return least <= band

    table_copies = [
        pltpu.make_async_copy(a, b, tab_load.at[i]) for i, (a, b) in enumerate([
            (inv_z_in, inv_z), (inv_y_in, inv_y), (inv_x_in, inv_x), (fwd_x_in, base_x), (fwd_y_in, fwd_y),
            (fwd_z_in, fwd_z)])
    ]
    table_copies[0].start()
    each(0, nch, lambda c: load_copy(c).start())
    for copy in table_copies[1:]:
        copy.start()

    barrier = pltpu.get_barrier_semaphore()
    each(1, n, lambda j: pl.semaphore_signal(
        barrier, inc=1, device_id={"fft": (me + j) % n}, device_id_type=MESH))
    each(1, m, lambda j: pl.semaphore_signal(
        barrier, inc=1, device_id={"scal": (mine + j) % m}, device_id_type=MESH))

    lane = lax.broadcasted_iota(jnp.int32, (half, 2 * length), 1) % length
    flip = jnp.where((lane % 2) * side == 1, -1.0, 1.0)
    kz_lane = jnp.where(lane < half, lane, lane - length).astype(f32)
    table_copies[0].wait()
    real_z = inv_z[:half].astype(f32) * flip
    imag_z = inv_z[half:].astype(f32) * flip
    zin[0:half] = real_z.astype(bf16)
    zin[half:length] = imag_z.astype(bf16)
    zin[length:length + half] = (-kz_lane * imag_z).astype(bf16)
    zin[length + half:] = (kz_lane * real_z).astype(bf16)

    pl.semaphore_wait(barrier, n + m - 2)

    def z_pair(pr, pair):
        res = dot(zin[...], pair)
        for k in range(2):
            for f in range(2):
                for p in range(2):
                    at = f * length + p * half
                    tmp[f, pl.ds(p * CHUNK + 2 * pr + k, half, stride=2 * CHUNK), :] = (
                        res[at:at + half, k * half:(k + 1) * half]
                    )

    def send_rows(kinds, h, c):
        both = jnp.concatenate([tmp[0].astype(bf16), tmp[1].astype(bf16)], axis=1)
        wsend[h, c] = both.reshape(sides, rows, 2 * CHUNK, 2 * half)
        for kind in kinds:
            each(1, sides, lambda j: row_copy(kind, h, c, (place + j) % sides, place).start())
        recv[place, h, c] = wsend[h, c, place]

    def begin(i):
        c = i % nch
        own = i < nch
        h = jnp.where(own, side, 1 - side)

        @pl.when(own)
        def _():
            load_copy(c).wait()

            def cast(r):
                tb[side, r] = out[:, r].astype(bf16)

            each(c * CHUNK, c * CHUNK + CHUNK, cast)
            swap_copy(c, side).start()

        @pl.when(jnp.logical_not(own))
        def _():
            swap_copy(c, 1 - side).wait_recv()

        for pr in range(CHUNK // 2):
            r = c * CHUNK + 2 * pr
            z_pair(pr, jnp.concatenate(
                [tb[h, r].reshape(2 * length, half), tb[h, r + 1].reshape(2 * length, half)], axis=1))
        send_rows((0, 1), h, c)

    each(0, nch, begin)
    each(1, m, lambda j: speed_copy((mine + j) % m, mine).start())
    own_speed().start()

    kx = lax.broadcasted_iota(jnp.int32, (length, half), 1).astype(f32)
    kz_row = lax.broadcasted_iota(jnp.int32, (length, half), 0)
    kz = jnp.where(kz_row < half, kz_row, kz_row - length).astype(f32)
    kxz = kx * kx + kz * kz
    weight = jnp.where(kx == 0.0, 1.0, 2.0)

    def ky_square(b, r):
        index = b * rows + r
        wave = jnp.where(index < half, index, index - length)
        return jnp.full((1, half), wave * wave, jnp.int32).astype(f32)

    acc[...] = jnp.zeros_like(acc)

    def add_row(r):
        real, imag = out[0, r], out[1, r]
        energy = weight * (real * real + imag * imag)
        acc[0] += jnp.sum(energy.reshape(length // 8, 8, half), axis=0)
        acc[1] += jnp.sum((energy * (kxz + ky_square(me, r))).reshape(length // 8, 8, half), axis=0)

    each(0, rows, add_row)

    col = lax.broadcasted_iota(jnp.int32, (length, 2 * length), 1)
    row_ky = ((col // (2 * CHUNK * nch * 2)) + ((col // (2 * CHUNK * nch)) % 2) * sides) * rows
    row_ky = row_ky + ((col // (2 * CHUNK)) % nch) * CHUNK + col % CHUNK
    row_ky = jnp.where(row_ky < half, row_ky, row_ky - length).astype(f32)
    for copy in table_copies[1:]:
        copy.wait()
    iny[:length] = (-row_ky * inv_y[length:].astype(f32)).astype(bf16)
    iny[length:] = (row_ky * inv_y[:length].astype(f32)).astype(bf16)
    for i in range(2):
        turn = base_x[:, i * half:(i + 1) * half].astype(f32)
        for p in range(4):
            fwd_x[p, :, i * half:(i + 1) * half] = (pltpu.roll(turn, p * quarter, 1) if p else turn).astype(bf16)
    kx_row = lax.broadcasted_iota(jnp.int32, (half, length), 0).astype(f32)
    inx[:half] = (kx_row * inv_x[half:].astype(f32)).astype(bf16)
    inx[half:] = (-kx_row * inv_x[:half].astype(f32)).astype(bf16)

    for h in range(2):
        for t in range(3):
            @pl.when(jnp.logical_not(needed(place + h * sides, t)))
            def _():
                def clear(j):
                    raw[h, (me + j) % n, :, t] = jnp.zeros((groups, 2, rows, half), bf16)

                each(1, n, clear)

    peak[...] = jnp.zeros_like(peak)

    each(nch, 2 * nch, begin)

    tile_lane = lax.broadcasted_iota(jnp.int32, (2 * length, half), 1) // quarter

    def pick(choices):
        result = choices[-1]
        for i in range(len(choices) - 2, -1, -1):
            result = jnp.where(tile_lane == i, choices[i], result)
        return result

    def planes_in(z):
        blocks = [recv[:, :, :, z + p].reshape(2 * length, 2 * half) for p in range(2)]
        section = dot(inv_y[...], jnp.concatenate(blocks, axis=1)).astype(bf16)
        turned = dot(iny[...], jnp.concatenate([b[:, :half] for b in blocks], axis=1)).astype(bf16)
        return section, turned

    def planes_out(st, z, hh, section, turned):
        halves = []
        for p in range(2):
            at = 2 * half * p
            sides_of = [
                (section[:, at:at + half], inx),
                (turned[:, half * p:half * (p + 1)], inv_x),
                (section[:, at + half:at + 2 * half], inv_x),
            ]
            total = None
            square = None
            for i, (part, table) in enumerate(sides_of):
                lhs = jnp.concatenate([part[:length], part[length:]], axis=1)
                grad = dot(lhs, table[...])
                u = uall[i, z + p].reshape(length, length).astype(f32)
                total = u * grad if total is None else total + u * grad
                if st == 0:
                    square = grad * grad if square is None else square + grad * grad
            if st == 0:
                peak[...] = jnp.maximum(peak[...], jnp.max(square.reshape(length // 8, 8, length), axis=0))
            flat = dot(total.astype(bf16), fwd_x[2 * hh + p]).astype(bf16)
            halves.append(jnp.concatenate([flat[:, :half], flat[:, half:]], axis=0))
        return jnp.concatenate(halves, axis=1)

    def for_blocks(st, d, act):
        if st == 0:
            each(0, 2, act)
        else:
            act(d // sides)

    def leave(st, low, high, own, across=None):
        def one(j):
            d = (me + jnp.where(side == st, j, n - j)) % n

            def send():
                h = d // sides if own else 1 - d // sides
                by_tiles(d % sides + h * sides, lambda k: each(
                    low, high, lambda g: forward_copy(st, g, d, h, me, k).start()))

            if across is None:
                send()
            else:
                pl.when((d // sides != side) if across else (d // sides == side))(send)

        each(1, n, one)

    def rows_arrive(kind):
        await_bytes(recv.at[pl.ds(0, sides - 1), :, :, planes_of(kind)], w_recv.at[kind])

    def rows_sent(kind):
        await_bytes(wsend.at[:, :, pl.ds(0, sides - 1), planes_of(kind)], w_send.at[kind])

    def run_group(st, g):
        inner = [planes_in(g * 4 + 2 * hh) for hh in range(2)]
        lines = [planes_out(st, g * 4 + 2 * hh, hh, *inner[hh]) for hh in range(2)]
        for hh in range(2):
            packed[hh] = dot(fwd_y[...], lines[hh])
        for t in range(3):
            chosen = [(i + 1 + t) % 4 for i in range(4)]
            tile = pick([packed[p // 2, :, (p % 2) * half:(p % 2 + 1) * half] for p in chosen]).astype(bf16)
            for q in range(2):
                fsend[:, g, t, q] = tile[q * length:(q + 1) * length].reshape(n, rows, half)

    def keep_own(g, h):
        raw[h, me, g] = fsend[place + h * sides, g]

    def group_arrive(st, g, h):
        by_tiles(place + h * sides, lambda k: await_bytes(
            raw.at[h, pl.ds(0, n - 1), g, pl.ds(0, k)], f_recv.at[st, g, h]))

    def forward_sent(st):
        def one(j):
            d = (me + j) % n

            def block(h):
                b = d % sides + h * sides
                by_tiles(b, lambda k: await_bytes(fsend.at[b, :, pl.ds(0, k)], f_send.at[h, d]))

            for_blocks(st, d, block)

        each(1, n, one)

    def row_pair(r, base, size):
        return jnp.concatenate(
            [tf[pl.ds(base + r + k, size, stride=rows), :].astype(bf16) for k in range(2)], axis=1)

    def unpack(st, h):
        def group(g):
            group_arrive(st, g, h)
            tiles = [raw[h, :, g, t].reshape(2 * length, half).astype(f32) for t in range(3)]
            for p in range(4):
                moved = [
                    pltpu.roll(tiles[t], (2 * t + 1 - p) % 4 * quarter, 1) if (2 * t + 1 - p) % 4 else tiles[t]
                    for t in range(3)
                ]
                at = pl.multiple_of((4 * g + p) * 2 * length, 2 * length)
                tf[pl.ds(at, 2 * length), :] = pick(moved + [jnp.zeros_like(tiles[0])])
            if st == 1:
                size = 2 * length // groups
                for i in range(rows // 2):
                    lined[i, pl.ds(pl.multiple_of(g * size, size), size)] = row_pair(2 * i, g * 8 * length, size)

        each(0, groups, group)

    await_bytes(uall.at[:, :, pl.ds(0, m - 1)], u_recv)
    own_speed().wait()

    def first_group(g):
        @pl.when(g == 0)
        def _():
            rows_arrive(0)

        @pl.when(g == lower)
        def _():
            rows_arrive(1)

        run_group(0, g)
        for h in range(2):
            keep_own(g, h)

        @pl.when(g < 2)
        def _():
            leave(0, g, g + 1, True)

    each(0, groups, first_group)

    line = lax.broadcasted_iota(jnp.int32, (8, 128), 0)
    largest = jnp.sqrt(jnp.max(peak[...], keepdims=True))
    local_var = jnp.sum(acc[0], keepdims=True) / cells
    local_grad = jnp.sum(acc[1], keepdims=True) / cells
    stat[...] = jnp.where(line == 0, local_var, jnp.where(line == 1, local_grad, largest))
    each(1, n, lambda j: stat_copy((me + j) % n, me).start())
    leave(0, 2, min(3, groups), True)
    outer = (place < sides // 2) == (side == 0)

    @pl.when(outer)
    def _():
        leave(0, min(3, groups), groups, True)
        leave(0, 0, groups, False)

    stats[me] = stat[...]
    rows_sent(0)
    rows_sent(1)
    await_bytes(stats.at[pl.ds(0, n - 1)], t_recv)
    @pl.when(jnp.logical_not(outer))
    def _():
        leave(0, min(3, groups), groups, True)
        leave(0, 0, groups, False, False)

    summed = jnp.sum(stats[...], axis=0)
    highest = jnp.max(stats[...], axis=0)
    kappa = ktable[species[0]] * highest[2:3, :1] * jnp.sqrt(summed[0:1, :1]) / (summed[1:2, :1] + 1e-06)
    kap[...] = jnp.broadcast_to(kappa, kap.shape)
    bound = jnp.full((1, half), bounds[0], jnp.int32).astype(f32)
    bound = bound * bound
    rate = -kappa * step_size

    def send_upper(h):
        for kind in uppers:
            each(1, sides, lambda j: block_copy(kind, h, (place + j) % sides, place).start())

    def second(h, c, own, inside):
        block = place + h * sides
        for pr in range(CHUNK // 2):
            r = c * CHUNK + 2 * pr
            moved = dot(fwd_z[...], row_pair(r, 0, 2 * length)) if inside else None
            cols = []
            for k in range(2):
                square = kxz + ky_square(block, r + k)
                factor = jnp.exp(rate * square)
                keep = square <= bound
                for p in range(2):
                    value = tb[h, r + k, p].astype(f32)
                    if inside:
                        add = moved[p * length:(p + 1) * length, k * half:(k + 1) * half]
                        add = jnp.where(keep, -step_size * add, 0.0)
                        value = value + add
                    cols.append((factor * value).astype(bf16))
                    if own:
                        start = out[p, r + k]
                        out[p, r + k] = factor * (start + 0.5 * add) if inside else factor * start
            z_pair(pr, jnp.concatenate(
                [jnp.concatenate(cols[:2], axis=0), jnp.concatenate(cols[2:], axis=0)], axis=1))
        send_rows((2,), h, c)

    def chunks(own, inside):
        h = side if own else 1 - side
        wanted = block_inside(h)

        @pl.when(wanted if inside else jnp.logical_not(wanted))
        def _():
            each(0, nch, lambda c: second(h, c, own, inside))
            if not inside:
                send_upper(h)

    for own in (True, False):
        chunks(own, False)
    for own in (True, False):
        unpack(0, side if own else 1 - side)
        if own:
            @pl.when(jnp.logical_not(outer))
            def _():
                leave(0, 0, groups, False, True)
        else:
            each(1, n, lambda j: pl.semaphore_signal(
                free, inc=1, device_id={"fft": (me + j) % n}, device_id_type=MESH))
        chunks(own, True)

    for h in range(2):
        @pl.when(block_inside(h))
        def _():
            send_upper(h)

    forward_sent(0)

    def last_group(g):
        @pl.when(g == 0)
        def _():
            rows_arrive(2)
            pl.semaphore_wait(free, n - 1)

        @pl.when(g >= lower)
        def _():
            rows_arrive(3 + g - lower)

        run_group(1, g)
        leave(1, g, g + 1, True)
        keep_own(g, side)

    each(0, groups, last_group)
    await_bytes(tb.at[side], x_send)
    await_bytes(uall.at[:, :, pl.ds(0, m - 1)], u_send)
    await_bytes(stats.at[pl.ds(0, n - 1)], t_send)
    for kind in (2, *uppers):
        rows_sent(kind)
    unpack(1, side)
    forward_sent(1)


def final_kernel(rows, length, partial, lined, kap, bounds, fwd_z_in, out, kap_out, fwd_z, done, t_load, d_out):
    half = length // 2
    f32 = jnp.float32
    step_size = cfl_number * 2.0 * math.pi / length
    pairs = rows // 2

    def each(act):
        def one(i, carry):
            act(i)
            return carry

        lax.fori_loop(0, pairs, one, 0, unroll=2)

    def done_copy(i):
        at = pl.ds(2 * i, 2)
        return pltpu.make_async_copy(done.at[:, at], out.at[:, at], d_out.at[i])

    table = pltpu.make_async_copy(fwd_z_in, fwd_z, t_load)
    table.start()

    kx = lax.broadcasted_iota(jnp.int32, (length, half), 1).astype(f32)
    kz = lax.broadcasted_iota(jnp.int32, (length, half), 0)
    kz = jnp.where(kz < half, kz, kz - length).astype(f32)
    bound = jnp.full((1, half), bounds[0], jnp.int32).astype(f32)
    kxz = kx * kx + kz * kz
    kap_out[0] = jnp.max(kap[...])
    table.wait()

    def pair(i):
        moved = dot(fwd_z[...], lined[i])
        for k in range(2):
            ky = lax.axis_index("fft") * rows + i * 2 + k
            ky = jnp.where(ky < half, ky, ky - length)
            keep = kxz + jnp.full((1, half), ky * ky, jnp.int32).astype(f32) <= bound * bound
            for p in range(2):
                value = moved[p * length:(p + 1) * length, k * half:(k + 1) * half]
                done[p, 2 * i + k] = partial[p, 2 * i + k] + jnp.where(keep, -0.5 * step_size * value, 0.0)
        done_copy(i).start()

    each(pair)
    each(lambda i: done_copy(i).wait())


def body(n, m, scalar_state, velocity, species, kappa_table, dealias_bound):
    rows = scalar_state.shape[2]
    length = scalar_state.shape[3]
    half = length // 2
    sides = n // 2
    nch = rows // CHUNK
    groups = rows // 4
    kinds = 3 + groups - groups // 2
    f32, bf16 = jnp.float32, jnp.bfloat16
    tables = lax.optimization_barrier(build_tables(length, n, rows))
    vmem = pl.BlockSpec(memory_space=pltpu.VMEM)
    smem = pl.BlockSpec(memory_space=pltpu.SMEM)
    hbm = pl.BlockSpec(memory_space=pl.ANY)
    dma = pltpu.SemaphoreType.DMA
    scratch = [pltpu.VMEM(t.shape, bf16) for t in tables] + [
        pltpu.VMEM((4, length, length), bf16),
        pltpu.VMEM((2, rows, 2, length, half), bf16),
        pltpu.VMEM((2, nch, sides, rows, 2 * CHUNK, 2 * half), bf16),
        pltpu.VMEM((sides, 2, nch, rows, 2 * CHUNK, 2 * half), bf16),
        pltpu.VMEM((2, half * 2 * CHUNK, half), f32),
        pltpu.VMEM((3, rows, m, length // m, length), bf16),
        pltpu.VMEM((n, groups, 3, 2, rows, half), bf16),
        pltpu.VMEM((2, n, groups, 3, 2, rows, half), bf16),
        pltpu.VMEM((2, 2 * length, 2 * half), f32),
        pltpu.VMEM((rows * 2 * length, half), f32),
        pltpu.VMEM((2 * length, 2 * length), bf16),
        pltpu.VMEM((2 * length, 2 * length), bf16),
        pltpu.VMEM((length, length), bf16),
        pltpu.VMEM((8, length), f32),
        pltpu.VMEM((2, 8, half), f32),
        pltpu.VMEM((8, 128), f32),
        pltpu.VMEM((n, 8, 128), f32),
        dma((nch,)), dma((len(tables),)), dma, dma((nch,)), dma((kinds,)), dma((kinds,)), dma, dma, dma,
        dma((2, n)), dma((2, groups, 2)), dma, dma,
        pltpu.SemaphoreType.REGULAR,
    ]
    partial, lined, kappa = pl.pallas_call(
        functools.partial(step_kernel, n, m, rows, length // 3),
        out_shape=[
            pltpu.VMEM((2, rows, length, half), f32),
            pltpu.VMEM((rows // 2, 2 * length, 2 * half), bf16),
            pltpu.VMEM((8, 128), f32),
        ],
        in_specs=[hbm, hbm, smem, smem, smem] + [hbm] * 6,
        out_specs=[vmem, vmem, vmem],
        scratch_shapes=scratch,
        compiler_params=pltpu.CompilerParams(
            collective_id=0, has_side_effects=True, vmem_limit_bytes=56 * 1024 * 1024,
        ),
        name="whole_step",
    )(scalar_state[0], velocity, species, kappa_table, dealias_bound, *tables)
    keep = functools.partial(pltpu.with_memory_space_constraint, memory_space=pltpu.VMEM)
    new_state, kappa = pl.pallas_call(
        functools.partial(final_kernel, rows, length),
        out_shape=[
            jax.ShapeDtypeStruct((2, rows, length, half), f32),
            jax.ShapeDtypeStruct((1,), f32),
        ],
        in_specs=[vmem, vmem, vmem, smem, hbm],
        out_specs=[hbm, smem],
        scratch_shapes=[
            pltpu.VMEM((2 * length, 2 * length), bf16),
            pltpu.VMEM((2, rows, length, half), f32),
            dma, dma((rows // 2,)),
        ],
        compiler_params=pltpu.CompilerParams(vmem_limit_bytes=24 * 1024 * 1024),
        name="final_step",
    )(keep(partial), keep(lined), keep(kappa), dealias_bound, tables[5])
    return new_state[None], kappa


def solution(mesh):
    placed = (
        P("scal", None, "fft", None, None),
        P(None, "fft", "scal", None),
        P("scal"),
        P(),
        P("scal"),
    )
    return jax.shard_map(
        functools.partial(body, mesh.shape["fft"], mesh.shape["scal"]),
        mesh=mesh,
        in_specs=placed,
        out_specs=(P("scal", None, "fft", None, None), P("scal")),
        check_vma=False,
    )
```

```python
import functools
import math

import numpy as np

import jax
import jax.numpy as jnp
from jax import lax
from jax.experimental import pallas as pl
from jax.experimental.pallas import tpu as pltpu
from jax.sharding import PartitionSpec as P

MESH = pl.DeviceIdType.MESH
cfl_number = 0.2
CHUNK = 4


def twiddle(size_in, size_out, length):
    row_index = np.arange(size_in, dtype=np.int32)[:, None]
    col_index = np.arange(size_out, dtype=np.int32)[None, :]
    angles = (row_index * col_index % length).astype(np.float32) * np.float32(2.0 * math.pi / length)
    norming = np.float32(1.0 / math.sqrt(length))
    return (np.cos(angles) * norming, np.sin(angles) * norming)


def build_tables(length, n, rows):
    half = length // 2
    quarter = half // 4
    sides = n // 2
    full_cos, full_sin = twiddle(length, length, length)
    inv_cos, inv_sin = twiddle(half, length, length)
    weight = np.where(np.arange(half) == 0, 1.0, 2.0).astype(np.float32)[:, None]
    fwd_cos, fwd_sin = twiddle(length, half, length)
    inv_z = np.block([[full_cos[:half], -full_sin[:half]], [full_sin[:half], full_cos[:half]]])
    inv_y = np.block([[full_cos, -full_sin], [full_sin, full_cos]])
    q, h, c, p, k = np.meshgrid(
        np.arange(sides), np.arange(2), np.arange(rows // CHUNK), np.arange(2), np.arange(CHUNK), indexing="ij"
    )
    inv_y = inv_y[:, ((q + h * sides) * rows + c * CHUNK + k + p * length).reshape(-1)]
    inv_x = np.concatenate([inv_cos * weight, -inv_sin * weight], axis=0)
    order = np.concatenate([(3 - l) * quarter + np.arange(quarter) for l in range(4)])
    fwd_x = np.concatenate([fwd_cos[:, order], -fwd_sin[:, order]], axis=1)
    fwd_y = np.block([[full_cos, full_sin], [-full_sin, full_cos]])
    z, s, p = np.meshgrid(np.arange(rows), np.arange(n), np.arange(2), indexing="ij")
    fwd_z = fwd_y[:, (s * rows + z + p * length).reshape(-1)]
    return tuple(
        jnp.asarray(t.astype(np.float32).astype(jnp.bfloat16)) for t in (inv_z, inv_y, inv_x, fwd_x, fwd_y, fwd_z)
    )


def dot(a, b):
    return jnp.dot(a, b, preferred_element_type=jnp.float32)


def step_kernel(n, m, rows, band, *refs):
    (state, vel, species, ktable, bounds, inv_z_in, inv_y_in, inv_x_in, fwd_x_in, fwd_y_in, fwd_z_in,
     out, lined, kap,
     inv_z, inv_y, inv_x, base_x, fwd_y, fwd_z, fwd_x, tb, wsend, recv, tmp, uall, fsend, raw, packed, tf, zin, iny, inx, peak, acc, stat, stats,
     s_load, tab_load, x_send, x_recv, w_send, w_recv, u_send, u_recv, u_loc,
     f_send, f_recv, t_send, t_recv, free) = refs
    length = n * rows
    half = length // 2
    quarter = half // 4
    sides = n // 2
    nch = rows // CHUNK
    groups = rows // 4
    f32 = jnp.float32
    bf16 = jnp.bfloat16
    step_size = cfl_number * 2.0 * math.pi / length
    cells = float(length) ** 3
    me = lax.axis_index("fft")
    mine = lax.axis_index("scal")
    side = me // sides
    place = me % sides
    partner = (me + sides) % n

    def each(low, high, act):
        def one(j, carry):
            act(j)
            return carry

        lax.fori_loop(low, high, one, 0)

    def load_copy(c):
        at = pl.ds(c * CHUNK, CHUNK)
        return pltpu.make_async_copy(state.at[:, at], out.at[:, at], s_load.at[c])

    def swap_copy(c, h):
        at = pl.ds(c * CHUNK, CHUNK)
        return pltpu.make_async_remote_copy(
            src_ref=tb.at[h, at], dst_ref=tb.at[h, at], send_sem=x_send, recv_sem=x_recv.at[c],
            device_id={"fft": partner}, device_id_type=MESH,
        )

    lower = groups - 1

    def planes_of(kind):
        if isinstance(kind, int) and kind in (0, 2):
            return pl.ds(0, lower * 4)
        if isinstance(kind, int) and kind == 1:
            return pl.ds(lower * 4, (groups - lower) * 4)
        return pl.ds((lower + kind - 3) * 4, 4)

    uppers = range(3, 3 + groups - lower)

    def row_copy(kind, h, c, to, slot):
        at = planes_of(kind)
        return pltpu.make_async_remote_copy(
            src_ref=wsend.at[h, c, to, at], dst_ref=recv.at[slot, h, c, at],
            send_sem=w_send.at[kind], recv_sem=w_recv.at[kind],
            device_id={"fft": side * sides + to}, device_id_type=MESH,
        )

    def block_copy(kind, h, to, slot):
        at = planes_of(kind)
        return pltpu.make_async_remote_copy(
            src_ref=wsend.at[h, :, to, at], dst_ref=recv.at[slot, h, :, at],
            send_sem=w_send.at[kind], recv_sem=w_recv.at[kind],
            device_id={"fft": side * sides + to}, device_id_type=MESH,
        )

    def speed_copy(s, slot):
        return pltpu.make_async_remote_copy(
            src_ref=vel, dst_ref=uall.at[:, :, slot], send_sem=u_send, recv_sem=u_recv,
            device_id={"scal": s}, device_id_type=MESH,
        )

    def own_speed():
        return pltpu.make_async_copy(vel, uall.at[:, :, mine], u_loc)

    def await_bytes(ref, sem):
        pltpu.make_async_copy(ref, ref, sem).wait()

    def forward_copy(st, g, d, h, slot, k):
        return pltpu.make_async_remote_copy(
            src_ref=fsend.at[d % sides + h * sides, g, pl.ds(0, k)], dst_ref=raw.at[h, slot, g, pl.ds(0, k)],
            send_sem=f_send.at[h, d], recv_sem=f_recv.at[st, g, h],
            device_id={"fft": d}, device_id_type=MESH,
        )

    def stat_copy(d, slot):
        return pltpu.make_async_remote_copy(
            src_ref=stat, dst_ref=stats.at[slot], send_sem=t_send, recv_sem=t_recv,
            device_id={"fft": d}, device_id_type=MESH,
        )

    def needed(b, t):
        low = b * rows
        least = jnp.where(low < half, low, length - low - rows + 1)
        return (t * quarter) ** 2 + least * least <= band * band

    def by_tiles(b, act):
        for k in range(1, 4):
            wanted = needed(b, k - 1)
            if k < 3:
                wanted = jnp.logical_and(wanted, jnp.logical_not(needed(b, k)))

            @pl.when(wanted)
            def _():
                act(k)

    def block_inside(h):
        low = (place + h * sides) * rows
        least = jnp.where(low < half, low, length - low - rows + 1)
        return least <= band

    table_copies = [
        pltpu.make_async_copy(a, b, tab_load.at[i]) for i, (a, b) in enumerate([
            (inv_z_in, inv_z), (inv_y_in, inv_y), (inv_x_in, inv_x), (fwd_x_in, base_x), (fwd_y_in, fwd_y),
            (fwd_z_in, fwd_z)])
    ]
    table_copies[0].start()
    each(0, nch, lambda c: load_copy(c).start())
    for copy in table_copies[1:]:
        copy.start()

    barrier = pltpu.get_barrier_semaphore()
    each(1, n, lambda j: pl.semaphore_signal(
        barrier, inc=1, device_id={"fft": (me + j) % n}, device_id_type=MESH))
    each(1, m, lambda j: pl.semaphore_signal(
        barrier, inc=1, device_id={"scal": (mine + j) % m}, device_id_type=MESH))

    lane = lax.broadcasted_iota(jnp.int32, (half, 2 * length), 1) % length
    flip = jnp.where((lane % 2) * side == 1, -1.0, 1.0)
    kz_lane = jnp.where(lane < half, lane, lane - length).astype(f32)
    table_copies[0].wait()
    real_z = inv_z[:half].astype(f32) * flip
    imag_z = inv_z[half:].astype(f32) * flip
    zin[0:half] = real_z.astype(bf16)
    zin[half:length] = imag_z.astype(bf16)
    zin[length:length + half] = (-kz_lane * imag_z).astype(bf16)
    zin[length + half:] = (kz_lane * real_z).astype(bf16)

    pl.semaphore_wait(barrier, n + m - 2)

    def z_pair(pr, pair):
        res = dot(zin[...], pair)
        for k in range(2):
            for f in range(2):
                for p in range(2):
                    at = f * length + p * half
                    tmp[f, pl.ds(p * CHUNK + 2 * pr + k, half, stride=2 * CHUNK), :] = (
                        res[at:at + half, k * half:(k + 1) * half]
                    )

    def send_rows(kinds, h, c):
        both = jnp.concatenate([tmp[0].astype(bf16), tmp[1].astype(bf16)], axis=1)
        wsend[h, c] = both.reshape(sides, rows, 2 * CHUNK, 2 * half)
        for kind in kinds:
            each(1, sides, lambda j: row_copy(kind, h, c, (place + j) % sides, place).start())
        recv[place, h, c] = wsend[h, c, place]

    def begin(i):
        c = i % nch
        own = i < nch
        h = jnp.where(own, side, 1 - side)

        @pl.when(own)
        def _():
            load_copy(c).wait()

            def cast(r):
                tb[side, r] = out[:, r].astype(bf16)

            each(c * CHUNK, c * CHUNK + CHUNK, cast)
            swap_copy(c, side).start()

        @pl.when(jnp.logical_not(own))
        def _():
            swap_copy(c, 1 - side).wait_recv()

        for pr in range(CHUNK // 2):
            r = c * CHUNK + 2 * pr
            z_pair(pr, jnp.concatenate(
                [tb[h, r].reshape(2 * length, half), tb[h, r + 1].reshape(2 * length, half)], axis=1))
        send_rows((0, 1), h, c)

    each(0, nch, begin)
    each(1, m, lambda j: speed_copy((mine + j) % m, mine).start())
    own_speed().start()

    kx = lax.broadcasted_iota(jnp.int32, (length, half), 1).astype(f32)
    kz_row = lax.broadcasted_iota(jnp.int32, (length, half), 0)
    kz = jnp.where(kz_row < half, kz_row, kz_row - length).astype(f32)
    kxz = kx * kx + kz * kz
    weight = jnp.where(kx == 0.0, 1.0, 2.0)

    def ky_square(b, r):
        index = b * rows + r
        wave = jnp.where(index < half, index, index - length)
        return jnp.full((1, half), wave * wave, jnp.int32).astype(f32)

    acc[...] = jnp.zeros_like(acc)

    def add_row(r):
        real, imag = out[0, r], out[1, r]
        energy = weight * (real * real + imag * imag)
        acc[0] += jnp.sum(energy.reshape(length // 8, 8, half), axis=0)
        acc[1] += jnp.sum((energy * (kxz + ky_square(me, r))).reshape(length // 8, 8, half), axis=0)

    each(0, rows, add_row)

    col = lax.broadcasted_iota(jnp.int32, (length, 2 * length), 1)
    row_ky = ((col // (2 * CHUNK * nch * 2)) + ((col // (2 * CHUNK * nch)) % 2) * sides) * rows
    row_ky = row_ky + ((col // (2 * CHUNK)) % nch) * CHUNK + col % CHUNK
    row_ky = jnp.where(row_ky < half, row_ky, row_ky - length).astype(f32)
    for copy in table_copies[1:]:
        copy.wait()
    iny[:length] = (-row_ky * inv_y[length:].astype(f32)).astype(bf16)
    iny[length:] = (row_ky * inv_y[:length].astype(f32)).astype(bf16)
    for i in range(2):
        turn = base_x[:, i * half:(i + 1) * half].astype(f32)
        for p in range(4):
            fwd_x[p, :, i * half:(i + 1) * half] = (pltpu.roll(turn, p * quarter, 1) if p else turn).astype(bf16)
    kx_row = lax.broadcasted_iota(jnp.int32, (half, length), 0).astype(f32)
    inx[:half] = (kx_row * inv_x[half:].astype(f32)).astype(bf16)
    inx[half:] = (-kx_row * inv_x[:half].astype(f32)).astype(bf16)

    for h in range(2):
        for t in range(3):
            @pl.when(jnp.logical_not(needed(place + h * sides, t)))
            def _():
                def clear(j):
                    raw[h, (me + j) % n, :, t] = jnp.zeros((groups, 2, rows, half), bf16)

                each(1, n, clear)

    peak[...] = jnp.zeros_like(peak)

    each(nch, 2 * nch, begin)

    tile_lane = lax.broadcasted_iota(jnp.int32, (2 * length, half), 1) // quarter

    def pick(choices):
        result = choices[-1]
        for i in range(len(choices) - 2, -1, -1):
            result = jnp.where(tile_lane == i, choices[i], result)
        return result

    def planes_in(z):
        blocks = [recv[:, :, :, z + p].reshape(2 * length, 2 * half) for p in range(2)]
        section = dot(inv_y[...], jnp.concatenate(blocks, axis=1)).astype(bf16)
        turned = dot(iny[...], jnp.concatenate([b[:, :half] for b in blocks], axis=1)).astype(bf16)
        return section, turned

    def planes_out(st, z, hh, section, turned):
        halves = []
        for p in range(2):
            at = 2 * half * p
            sides_of = [
                (section[:, at:at + half], inx),
                (turned[:, half * p:half * (p + 1)], inv_x),
                (section[:, at + half:at + 2 * half], inv_x),
            ]
            total = None
            square = None
            for i, (part, table) in enumerate(sides_of):
                lhs = jnp.concatenate([part[:length], part[length:]], axis=1)
                grad = dot(lhs, table[...])
                u = uall[i, z + p].reshape(length, length).astype(f32)
                total = u * grad if total is None else total + u * grad
                if st == 0:
                    square = grad * grad if square is None else square + grad * grad
            if st == 0:
                peak[...] = jnp.maximum(peak[...], jnp.max(square.reshape(length // 8, 8, length), axis=0))
            flat = dot(total.astype(bf16), fwd_x[2 * hh + p]).astype(bf16)
            halves.append(jnp.concatenate([flat[:, :half], flat[:, half:]], axis=0))
        return jnp.concatenate(halves, axis=1)

    def for_blocks(st, d, act):
        if st == 0:
            each(0, 2, act)
        else:
            act(d // sides)

    def leave(st, low, high, own):
        def one(j):
            d = (me + jnp.where(side == 0, j, n - j)) % n
            h = d // sides if own else 1 - d // sides
            by_tiles(d % sides + h * sides, lambda k: each(
                low, high, lambda g: forward_copy(st, g, d, h, me, k).start()))

        each(1, n, one)

    def rows_arrive(kind):
        await_bytes(recv.at[pl.ds(0, sides - 1), :, :, planes_of(kind)], w_recv.at[kind])

    def rows_sent(kind):
        await_bytes(wsend.at[:, :, pl.ds(0, sides - 1), planes_of(kind)], w_send.at[kind])

    def run_group(st, g):
        inner = [planes_in(g * 4 + 2 * hh) for hh in range(2)]
        lines = [planes_out(st, g * 4 + 2 * hh, hh, *inner[hh]) for hh in range(2)]
        for hh in range(2):
            packed[hh] = dot(fwd_y[...], lines[hh])
        for t in range(3):
            chosen = [(i + 1 + t) % 4 for i in range(4)]
            tile = pick([packed[p // 2, :, (p % 2) * half:(p % 2 + 1) * half] for p in chosen]).astype(bf16)
            for q in range(2):
                fsend[:, g, t, q] = tile[q * length:(q + 1) * length].reshape(n, rows, half)

    def keep_own(g, h):
        raw[h, me, g] = fsend[place + h * sides, g]

    def group_arrive(st, g, h):
        by_tiles(place + h * sides, lambda k: await_bytes(
            raw.at[h, pl.ds(0, n - 1), g, pl.ds(0, k)], f_recv.at[st, g, h]))

    def forward_sent(st):
        def one(j):
            d = (me + j) % n

            def block(h):
                b = d % sides + h * sides
                by_tiles(b, lambda k: await_bytes(fsend.at[b, :, pl.ds(0, k)], f_send.at[h, d]))

            for_blocks(st, d, block)

        each(1, n, one)

    def row_pair(r, base, size):
        return jnp.concatenate(
            [tf[pl.ds(base + r + k, size, stride=rows), :].astype(bf16) for k in range(2)], axis=1)

    def unpack(st, h):
        def group(g):
            group_arrive(st, g, h)
            tiles = [raw[h, :, g, t].reshape(2 * length, half).astype(f32) for t in range(3)]
            for p in range(4):
                moved = [
                    pltpu.roll(tiles[t], (2 * t + 1 - p) % 4 * quarter, 1) if (2 * t + 1 - p) % 4 else tiles[t]
                    for t in range(3)
                ]
                at = pl.multiple_of((4 * g + p) * 2 * length, 2 * length)
                tf[pl.ds(at, 2 * length), :] = pick(moved + [jnp.zeros_like(tiles[0])])
            if st == 1:
                size = 2 * length // groups
                for i in range(rows // 2):
                    lined[i, pl.ds(pl.multiple_of(g * size, size), size)] = row_pair(2 * i, g * 8 * length, size)

        each(0, groups, group)

    await_bytes(uall.at[:, :, pl.ds(0, m - 1)], u_recv)
    own_speed().wait()

    def first_group(g):
        @pl.when(g == 0)
        def _():
            rows_arrive(0)

        @pl.when(g == lower)
        def _():
            rows_arrive(1)

        run_group(0, g)
        for h in range(2):
            keep_own(g, h)

        @pl.when(g < 2)
        def _():
            leave(0, g, g + 1, True)

    each(0, groups, first_group)

    line = lax.broadcasted_iota(jnp.int32, (8, 128), 0)
    largest = jnp.sqrt(jnp.max(peak[...], keepdims=True))
    local_var = jnp.sum(acc[0], keepdims=True) / cells
    local_grad = jnp.sum(acc[1], keepdims=True) / cells
    stat[...] = jnp.where(line == 0, local_var, jnp.where(line == 1, local_grad, largest))
    each(1, n, lambda j: stat_copy((me + j) % n, me).start())
    leave(0, 2, groups, True)
    leave(0, 0, groups, False)
    stats[me] = stat[...]
    rows_sent(0)
    rows_sent(1)
    await_bytes(stats.at[pl.ds(0, n - 1)], t_recv)
    summed = jnp.sum(stats[...], axis=0)
    highest = jnp.max(stats[...], axis=0)
    kappa = ktable[species[0]] * highest[2:3, :1] * jnp.sqrt(summed[0:1, :1]) / (summed[1:2, :1] + 1e-06)
    kap[...] = jnp.broadcast_to(kappa, kap.shape)
    bound = jnp.full((1, half), bounds[0], jnp.int32).astype(f32)
    bound = bound * bound
    rate = -kappa * step_size

    def send_upper(h):
        for kind in uppers:
            each(1, sides, lambda j: block_copy(kind, h, (place + j) % sides, place).start())

    def second(h, c, own, inside):
        block = place + h * sides
        for pr in range(CHUNK // 2):
            r = c * CHUNK + 2 * pr
            moved = dot(fwd_z[...], row_pair(r, 0, 2 * length)) if inside else None
            cols = []
            for k in range(2):
                square = kxz + ky_square(block, r + k)
                factor = jnp.exp(rate * square)
                keep = square <= bound
                for p in range(2):
                    value = tb[h, r + k, p].astype(f32)
                    if inside:
                        add = moved[p * length:(p + 1) * length, k * half:(k + 1) * half]
                        add = jnp.where(keep, -step_size * add, 0.0)
                        value = value + add
                    cols.append((factor * value).astype(bf16))
                    if own:
                        start = out[p, r + k]
                        out[p, r + k] = factor * (start + 0.5 * add) if inside else factor * start
            z_pair(pr, jnp.concatenate(
                [jnp.concatenate(cols[:2], axis=0), jnp.concatenate(cols[2:], axis=0)], axis=1))
        send_rows((2,), h, c)

    def chunks(own, inside):
        h = side if own else 1 - side
        wanted = block_inside(h)

        @pl.when(wanted if inside else jnp.logical_not(wanted))
        def _():
            each(0, nch, lambda c: second(h, c, own, inside))
            if not inside:
                send_upper(h)

    for own in (True, False):
        chunks(own, False)
    for own in (True, False):
        unpack(0, side if own else 1 - side)
        if not own:
            each(1, n, lambda j: pl.semaphore_signal(
                free, inc=1, device_id={"fft": (me + j) % n}, device_id_type=MESH))
        chunks(own, True)

    for h in range(2):
        @pl.when(block_inside(h))
        def _():
            send_upper(h)

    forward_sent(0)

    def last_group(g):
        @pl.when(g == 0)
        def _():
            rows_arrive(2)
            pl.semaphore_wait(free, n - 1)

        @pl.when(g >= lower)
        def _():
            rows_arrive(3 + g - lower)

        run_group(1, g)
        leave(1, g, g + 1, True)
        keep_own(g, side)

    each(0, groups, last_group)
    await_bytes(tb.at[side], x_send)
    await_bytes(uall.at[:, :, pl.ds(0, m - 1)], u_send)
    await_bytes(stats.at[pl.ds(0, n - 1)], t_send)
    for kind in (2, *uppers):
        rows_sent(kind)
    unpack(1, side)
    forward_sent(1)


def final_kernel(rows, length, partial, lined, kap, bounds, fwd_z_in, out, kap_out, fwd_z, done, t_load, d_out):
    half = length // 2
    f32 = jnp.float32
    step_size = cfl_number * 2.0 * math.pi / length
    pairs = rows // 2

    def each(act):
        def one(i, carry):
            act(i)
            return carry

        lax.fori_loop(0, pairs, one, 0, unroll=4)

    def done_copy(i):
        at = pl.ds(2 * i, 2)
        return pltpu.make_async_copy(done.at[:, at], out.at[:, at], d_out.at[i])

    table = pltpu.make_async_copy(fwd_z_in, fwd_z, t_load)
    table.start()

    kx = lax.broadcasted_iota(jnp.int32, (length, half), 1).astype(f32)
    kz = lax.broadcasted_iota(jnp.int32, (length, half), 0)
    kz = jnp.where(kz < half, kz, kz - length).astype(f32)
    bound = jnp.full((1, half), bounds[0], jnp.int32).astype(f32)
    kxz = kx * kx + kz * kz
    kap_out[0] = jnp.max(kap[...])
    table.wait()

    def pair(i):
        moved = dot(fwd_z[...], lined[i])
        for k in range(2):
            ky = lax.axis_index("fft") * rows + i * 2 + k
            ky = jnp.where(ky < half, ky, ky - length)
            keep = kxz + jnp.full((1, half), ky * ky, jnp.int32).astype(f32) <= bound * bound
            for p in range(2):
                value = moved[p * length:(p + 1) * length, k * half:(k + 1) * half]
                done[p, 2 * i + k] = partial[p, 2 * i + k] + jnp.where(keep, -0.5 * step_size * value, 0.0)
        done_copy(i).start()

    each(pair)
    each(lambda i: done_copy(i).wait())


def body(n, m, scalar_state, velocity, species, kappa_table, dealias_bound):
    rows = scalar_state.shape[2]
    length = scalar_state.shape[3]
    half = length // 2
    sides = n // 2
    nch = rows // CHUNK
    groups = rows // 4
    kinds = 4
    f32, bf16 = jnp.float32, jnp.bfloat16
    tables = lax.optimization_barrier(build_tables(length, n, rows))
    vmem = pl.BlockSpec(memory_space=pltpu.VMEM)
    smem = pl.BlockSpec(memory_space=pltpu.SMEM)
    hbm = pl.BlockSpec(memory_space=pl.ANY)
    dma = pltpu.SemaphoreType.DMA
    scratch = [pltpu.VMEM(t.shape, bf16) for t in tables] + [
        pltpu.VMEM((4, length, length), bf16),
        pltpu.VMEM((2, rows, 2, length, half), bf16),
        pltpu.VMEM((2, nch, sides, rows, 2 * CHUNK, 2 * half), bf16),
        pltpu.VMEM((sides, 2, nch, rows, 2 * CHUNK, 2 * half), bf16),
        pltpu.VMEM((2, half * 2 * CHUNK, half), f32),
        pltpu.VMEM((3, rows, m, length // m, length), bf16),
        pltpu.VMEM((n, groups, 3, 2, rows, half), bf16),
        pltpu.VMEM((2, n, groups, 3, 2, rows, half), bf16),
        pltpu.VMEM((2, 2 * length, 2 * half), f32),
        pltpu.VMEM((rows * 2 * length, half), f32),
        pltpu.VMEM((2 * length, 2 * length), bf16),
        pltpu.VMEM((2 * length, 2 * length), bf16),
        pltpu.VMEM((length, length), bf16),
        pltpu.VMEM((8, length), f32),
        pltpu.VMEM((2, 8, half), f32),
        pltpu.VMEM((8, 128), f32),
        pltpu.VMEM((n, 8, 128), f32),
        dma((nch,)), dma((len(tables),)), dma, dma((nch,)), dma((kinds,)), dma((kinds,)), dma, dma, dma,
        dma((2, n)), dma((2, groups, 2)), dma, dma,
        pltpu.SemaphoreType.REGULAR,
    ]
    partial, lined, kappa = pl.pallas_call(
        functools.partial(step_kernel, n, m, rows, length // 3),
        out_shape=[
            pltpu.VMEM((2, rows, length, half), f32),
            pltpu.VMEM((rows // 2, 2 * length, 2 * half), bf16),
            pltpu.VMEM((8, 128), f32),
        ],
        in_specs=[hbm, hbm, smem, smem, smem] + [hbm] * 6,
        out_specs=[vmem, vmem, vmem],
        scratch_shapes=scratch,
        compiler_params=pltpu.CompilerParams(
            collective_id=0, has_side_effects=True, vmem_limit_bytes=56 * 1024 * 1024,
        ),
        name="whole_step",
    )(scalar_state[0], velocity, species, kappa_table, dealias_bound, *tables)
    keep = functools.partial(pltpu.with_memory_space_constraint, memory_space=pltpu.VMEM)
    new_state, kappa = pl.pallas_call(
        functools.partial(final_kernel, rows, length),
        out_shape=[
            jax.ShapeDtypeStruct((2, rows, length, half), f32),
            jax.ShapeDtypeStruct((1,), f32),
        ],
        in_specs=[vmem, vmem, vmem, smem, hbm],
        out_specs=[hbm, smem],
        scratch_shapes=[
            pltpu.VMEM((2 * length, 2 * length), bf16),
            pltpu.VMEM((2, rows, length, half), f32),
            dma, dma((rows // 2,)),
        ],
        compiler_params=pltpu.CompilerParams(vmem_limit_bytes=24 * 1024 * 1024),
        name="final_step",
    )(keep(partial), keep(lined), keep(kappa), dealias_bound, tables[5])
    return new_state[None], kappa


def solution(mesh):
    placed = (
        P("scal", None, "fft", None, None),
        P(None, "fft", "scal", None),
        P("scal"),
        P(),
        P("scal"),
    )
    return jax.shard_map(
        functools.partial(body, mesh.shape["fft"], mesh.shape["scal"]),
        mesh=mesh,
        in_specs=placed,
        out_specs=(P("scal", None, "fft", None, None), P("scal")),
        check_vma=False,
    )
```

```python
import functools
import math

import numpy as np

import jax
import jax.numpy as jnp
from jax import lax
from jax.experimental import pallas as pl
from jax.experimental.pallas import tpu as pltpu
from jax.sharding import PartitionSpec as P

MESH = pl.DeviceIdType.MESH
cfl_number = 0.2
CHUNK = 4


def twiddle(size_in, size_out, length):
    row_index = np.arange(size_in, dtype=np.int32)[:, None]
    col_index = np.arange(size_out, dtype=np.int32)[None, :]
    angles = (row_index * col_index % length).astype(np.float32) * np.float32(2.0 * math.pi / length)
    norming = np.float32(1.0 / math.sqrt(length))
    return (np.cos(angles) * norming, np.sin(angles) * norming)


def build_tables(length, n, rows):
    half = length // 2
    quarter = half // 4
    sides = n // 2
    full_cos, full_sin = twiddle(length, length, length)
    inv_cos, inv_sin = twiddle(half, length, length)
    weight = np.where(np.arange(half) == 0, 1.0, 2.0).astype(np.float32)[:, None]
    fwd_cos, fwd_sin = twiddle(length, half, length)
    inv_z = np.block([[full_cos[:half], -full_sin[:half]], [full_sin[:half], full_cos[:half]]])
    inv_y = np.block([[full_cos, -full_sin], [full_sin, full_cos]])
    q, h, c, p, k = np.meshgrid(
        np.arange(sides), np.arange(2), np.arange(rows // CHUNK), np.arange(2), np.arange(CHUNK), indexing="ij"
    )
    inv_y = inv_y[:, ((q + h * sides) * rows + c * CHUNK + k + p * length).reshape(-1)]
    inv_x = np.concatenate([inv_cos * weight, -inv_sin * weight], axis=0)
    order = np.concatenate([(3 - l) * quarter + np.arange(quarter) for l in range(4)])
    fwd_x = np.concatenate([fwd_cos[:, order], -fwd_sin[:, order]], axis=1)
    fwd_y = np.block([[full_cos, full_sin], [-full_sin, full_cos]])
    z, s, p = np.meshgrid(np.arange(rows), np.arange(n), np.arange(2), indexing="ij")
    fwd_z = fwd_y[:, (s * rows + z + p * length).reshape(-1)]
    return tuple(
        jnp.asarray(t.astype(np.float32).astype(jnp.bfloat16)) for t in (inv_z, inv_y, inv_x, fwd_x, fwd_y, fwd_z)
    )


def dot(a, b):
    return jnp.dot(a, b, preferred_element_type=jnp.float32)


def step_kernel(n, m, rows, band, *refs):
    (state, vel, species, ktable, bounds, inv_z_in, inv_y_in, inv_x_in, fwd_x_in, fwd_y_in, fwd_z_in,
     out, lined, kap,
     inv_z, inv_y, inv_x, base_x, fwd_y, fwd_z, fwd_x, tb, wsend, recv, tmp, uall, fsend, raw, packed, tf, zin, iny, inx, peak, acc, stat, stats,
     s_load, tab_load, x_send, x_recv, w_send, w_recv, u_send, u_recv, u_loc,
     f_send, f_recv, t_send, t_recv, free) = refs
    length = n * rows
    half = length // 2
    quarter = half // 4
    sides = n // 2
    nch = rows // CHUNK
    groups = rows // 4
    f32 = jnp.float32
    bf16 = jnp.bfloat16
    step_size = cfl_number * 2.0 * math.pi / length
    cells = float(length) ** 3
    me = lax.axis_index("fft")
    mine = lax.axis_index("scal")
    side = me // sides
    place = me % sides
    partner = (me + sides) % n

    def each(low, high, act):
        def one(j, carry):
            act(j)
            return carry

        lax.fori_loop(low, high, one, 0)

    def load_copy(c):
        at = pl.ds(c * CHUNK, CHUNK)
        return pltpu.make_async_copy(state.at[:, at], out.at[:, at], s_load.at[c])

    def swap_copy(c, h):
        at = pl.ds(c * CHUNK, CHUNK)
        return pltpu.make_async_remote_copy(
            src_ref=tb.at[h, at], dst_ref=tb.at[h, at], send_sem=x_send, recv_sem=x_recv.at[c],
            device_id={"fft": partner}, device_id_type=MESH,
        )

    lower = groups - 1

    def planes_of(kind):
        if isinstance(kind, int) and kind in (0, 2):
            return pl.ds(0, lower * 4)
        if isinstance(kind, int) and kind == 1:
            return pl.ds(lower * 4, (groups - lower) * 4)
        return pl.ds((lower + kind - 3) * 4, 4)

    uppers = range(3, 3 + groups - lower)

    def row_copy(kind, h, c, to, slot):
        at = planes_of(kind)
        return pltpu.make_async_remote_copy(
            src_ref=wsend.at[h, c, to, at], dst_ref=recv.at[slot, h, c, at],
            send_sem=w_send.at[kind], recv_sem=w_recv.at[kind],
            device_id={"fft": side * sides + to}, device_id_type=MESH,
        )

    def block_copy(kind, h, to, slot):
        at = planes_of(kind)
        return pltpu.make_async_remote_copy(
            src_ref=wsend.at[h, :, to, at], dst_ref=recv.at[slot, h, :, at],
            send_sem=w_send.at[kind], recv_sem=w_recv.at[kind],
            device_id={"fft": side * sides + to}, device_id_type=MESH,
        )

    def speed_copy(s, slot):
        return pltpu.make_async_remote_copy(
            src_ref=vel, dst_ref=uall.at[:, :, slot], send_sem=u_send, recv_sem=u_recv,
            device_id={"scal": s}, device_id_type=MESH,
        )

    def own_speed():
        return pltpu.make_async_copy(vel, uall.at[:, :, mine], u_loc)

    def await_bytes(ref, sem):
        pltpu.make_async_copy(ref, ref, sem).wait()

    def forward_copy(st, g, d, h, slot, k):
        return pltpu.make_async_remote_copy(
            src_ref=fsend.at[d % sides + h * sides, g, pl.ds(0, k)], dst_ref=raw.at[h, slot, g, pl.ds(0, k)],
            send_sem=f_send.at[h, d], recv_sem=f_recv.at[st, g, h],
            device_id={"fft": d}, device_id_type=MESH,
        )

    def stat_copy(d, slot):
        return pltpu.make_async_remote_copy(
            src_ref=stat, dst_ref=stats.at[slot], send_sem=t_send, recv_sem=t_recv,
            device_id={"fft": d}, device_id_type=MESH,
        )

    def needed(b, t):
        low = b * rows
        least = jnp.where(low < half, low, length - low - rows + 1)
        return (t * quarter) ** 2 + least * least <= band * band

    def by_tiles(b, act):
        for k in range(1, 4):
            wanted = needed(b, k - 1)
            if k < 3:
                wanted = jnp.logical_and(wanted, jnp.logical_not(needed(b, k)))

            @pl.when(wanted)
            def _():
                act(k)

    def block_inside(h):
        low = (place + h * sides) * rows
        least = jnp.where(low < half, low, length - low - rows + 1)
        return least <= band

    table_copies = [
        pltpu.make_async_copy(a, b, tab_load.at[i]) for i, (a, b) in enumerate([
            (inv_z_in, inv_z), (inv_y_in, inv_y), (inv_x_in, inv_x), (fwd_x_in, base_x), (fwd_y_in, fwd_y),
            (fwd_z_in, fwd_z)])
    ]
    table_copies[0].start()
    each(0, nch, lambda c: load_copy(c).start())
    for copy in table_copies[1:]:
        copy.start()

    barrier = pltpu.get_barrier_semaphore()
    each(1, n, lambda j: pl.semaphore_signal(
        barrier, inc=1, device_id={"fft": (me + j) % n}, device_id_type=MESH))
    each(1, m, lambda j: pl.semaphore_signal(
        barrier, inc=1, device_id={"scal": (mine + j) % m}, device_id_type=MESH))

    lane = lax.broadcasted_iota(jnp.int32, (half, 2 * length), 1) % length
    flip = jnp.where((lane % 2) * side == 1, -1.0, 1.0)
    kz_lane = jnp.where(lane < half, lane, lane - length).astype(f32)
    table_copies[0].wait()
    real_z = inv_z[:half].astype(f32) * flip
    imag_z = inv_z[half:].astype(f32) * flip
    zin[0:half] = real_z.astype(bf16)
    zin[half:length] = imag_z.astype(bf16)
    zin[length:length + half] = (-kz_lane * imag_z).astype(bf16)
    zin[length + half:] = (kz_lane * real_z).astype(bf16)

    pl.semaphore_wait(barrier, n + m - 2)

    def z_pair(pr, pair):
        res = dot(zin[...], pair)
        for k in range(2):
            for f in range(2):
                for p in range(2):
                    at = f * length + p * half
                    tmp[f, pl.ds(p * CHUNK + 2 * pr + k, half, stride=2 * CHUNK), :] = (
                        res[at:at + half, k * half:(k + 1) * half]
                    )

    def send_rows(kinds, h, c):
        both = jnp.concatenate([tmp[0].astype(bf16), tmp[1].astype(bf16)], axis=1)
        wsend[h, c] = both.reshape(sides, rows, 2 * CHUNK, 2 * half)
        for kind in kinds:
            each(1, sides, lambda j: row_copy(kind, h, c, (place + j) % sides, place).start())
        recv[place, h, c] = wsend[h, c, place]

    def begin(i):
        c = i % nch
        own = i < nch
        h = jnp.where(own, side, 1 - side)

        @pl.when(own)
        def _():
            load_copy(c).wait()

            def cast(r):
                tb[side, r] = out[:, r].astype(bf16)

            each(c * CHUNK, c * CHUNK + CHUNK, cast)
            swap_copy(c, side).start()

        @pl.when(jnp.logical_not(own))
        def _():
            swap_copy(c, 1 - side).wait_recv()

        for pr in range(CHUNK // 2):
            r = c * CHUNK + 2 * pr
            z_pair(pr, jnp.concatenate(
                [tb[h, r].reshape(2 * length, half), tb[h, r + 1].reshape(2 * length, half)], axis=1))
        send_rows((0, 1), h, c)

    each(0, nch, begin)
    each(1, m, lambda j: speed_copy((mine + j) % m, mine).start())
    own_speed().start()

    kx = lax.broadcasted_iota(jnp.int32, (length, half), 1).astype(f32)
    kz_row = lax.broadcasted_iota(jnp.int32, (length, half), 0)
    kz = jnp.where(kz_row < half, kz_row, kz_row - length).astype(f32)
    kxz = kx * kx + kz * kz
    weight = jnp.where(kx == 0.0, 1.0, 2.0)

    def ky_square(b, r):
        index = b * rows + r
        wave = jnp.where(index < half, index, index - length)
        return jnp.full((1, half), wave * wave, jnp.int32).astype(f32)

    acc[...] = jnp.zeros_like(acc)

    def add_row(r):
        real, imag = out[0, r], out[1, r]
        energy = weight * (real * real + imag * imag)
        acc[0] += jnp.sum(energy.reshape(length // 8, 8, half), axis=0)
        acc[1] += jnp.sum((energy * (kxz + ky_square(me, r))).reshape(length // 8, 8, half), axis=0)

    each(0, rows, add_row)

    col = lax.broadcasted_iota(jnp.int32, (length, 2 * length), 1)
    row_ky = ((col // (2 * CHUNK * nch * 2)) + ((col // (2 * CHUNK * nch)) % 2) * sides) * rows
    row_ky = row_ky + ((col // (2 * CHUNK)) % nch) * CHUNK + col % CHUNK
    row_ky = jnp.where(row_ky < half, row_ky, row_ky - length).astype(f32)
    for copy in table_copies[1:]:
        copy.wait()
    iny[:length] = (-row_ky * inv_y[length:].astype(f32)).astype(bf16)
    iny[length:] = (row_ky * inv_y[:length].astype(f32)).astype(bf16)
    for i in range(2):
        turn = base_x[:, i * half:(i + 1) * half].astype(f32)
        for p in range(4):
            fwd_x[p, :, i * half:(i + 1) * half] = (pltpu.roll(turn, p * quarter, 1) if p else turn).astype(bf16)
    kx_row = lax.broadcasted_iota(jnp.int32, (half, length), 0).astype(f32)
    inx[:half] = (kx_row * inv_x[half:].astype(f32)).astype(bf16)
    inx[half:] = (-kx_row * inv_x[:half].astype(f32)).astype(bf16)

    for h in range(2):
        for t in range(3):
            @pl.when(jnp.logical_not(needed(place + h * sides, t)))
            def _():
                def clear(j):
                    raw[h, (me + j) % n, :, t] = jnp.zeros((groups, 2, rows, half), bf16)

                each(1, n, clear)

    peak[...] = jnp.zeros_like(peak)

    each(nch, 2 * nch, begin)

    tile_lane = lax.broadcasted_iota(jnp.int32, (2 * length, half), 1) // quarter

    def pick(choices):
        result = choices[-1]
        for i in range(len(choices) - 2, -1, -1):
            result = jnp.where(tile_lane == i, choices[i], result)
        return result

    def planes_in(z):
        blocks = [recv[:, :, :, z + p].reshape(2 * length, 2 * half) for p in range(2)]
        section = dot(inv_y[...], jnp.concatenate(blocks, axis=1)).astype(bf16)
        turned = dot(iny[...], jnp.concatenate([b[:, :half] for b in blocks], axis=1)).astype(bf16)
        return section, turned

    def planes_out(st, z, hh, section, turned):
        halves = []
        for p in range(2):
            at = 2 * half * p
            sides_of = [
                (section[:, at:at + half], inx),
                (turned[:, half * p:half * (p + 1)], inv_x),
                (section[:, at + half:at + 2 * half], inv_x),
            ]
            total = None
            square = None
            for i, (part, table) in enumerate(sides_of):
                lhs = jnp.concatenate([part[:length], part[length:]], axis=1)
                grad = dot(lhs, table[...])
                u = uall[i, z + p].reshape(length, length).astype(f32)
                total = u * grad if total is None else total + u * grad
                if st == 0:
                    square = grad * grad if square is None else square + grad * grad
            if st == 0:
                peak[...] = jnp.maximum(peak[...], jnp.max(square.reshape(length // 8, 8, length), axis=0))
            flat = dot(total.astype(bf16), fwd_x[2 * hh + p]).astype(bf16)
            halves.append(jnp.concatenate([flat[:, :half], flat[:, half:]], axis=0))
        return jnp.concatenate(halves, axis=1)

    def for_blocks(st, d, act):
        if st == 0:
            each(0, 2, act)
        else:
            act(d // sides)

    def leave(st, low, high, own):
        def one(j):
            d = (me + jnp.where(side == 0, j, n - j)) % n
            h = d // sides if own else 1 - d // sides
            by_tiles(d % sides + h * sides, lambda k: each(
                low, high, lambda g: forward_copy(st, g, d, h, me, k).start()))

        each(1, n, one)

    def rows_arrive(kind):
        await_bytes(recv.at[pl.ds(0, sides - 1), :, :, planes_of(kind)], w_recv.at[kind])

    def rows_sent(kind):
        await_bytes(wsend.at[:, :, pl.ds(0, sides - 1), planes_of(kind)], w_send.at[kind])

    def run_group(st, g):
        inner = [planes_in(g * 4 + 2 * hh) for hh in range(2)]
        lines = [planes_out(st, g * 4 + 2 * hh, hh, *inner[hh]) for hh in range(2)]
        for hh in range(2):
            packed[hh] = dot(fwd_y[...], lines[hh])
        for t in range(3):
            chosen = [(i + 1 + t) % 4 for i in range(4)]
            tile = pick([packed[p // 2, :, (p % 2) * half:(p % 2 + 1) * half] for p in chosen]).astype(bf16)
            for q in range(2):
                fsend[:, g, t, q] = tile[q * length:(q + 1) * length].reshape(n, rows, half)

    def keep_own(g, h):
        raw[h, me, g] = fsend[place + h * sides, g]

    def group_arrive(st, g, h):
        by_tiles(place + h * sides, lambda k: await_bytes(
            raw.at[h, pl.ds(0, n - 1), g, pl.ds(0, k)], f_recv.at[st, g, h]))

    def forward_sent(st):
        def one(j):
            d = (me + j) % n

            def block(h):
                b = d % sides + h * sides
                by_tiles(b, lambda k: await_bytes(fsend.at[b, :, pl.ds(0, k)], f_send.at[h, d]))

            for_blocks(st, d, block)

        each(1, n, one)

    def row_pair(r, base, size):
        return jnp.concatenate(
            [tf[pl.ds(base + r + k, size, stride=rows), :].astype(bf16) for k in range(2)], axis=1)

    def unpack(st, h):
        def group(g):
            group_arrive(st, g, h)
            tiles = [raw[h, :, g, t].reshape(2 * length, half).astype(f32) for t in range(3)]
            for p in range(4):
                moved = [
                    pltpu.roll(tiles[t], (2 * t + 1 - p) % 4 * quarter, 1) if (2 * t + 1 - p) % 4 else tiles[t]
                    for t in range(3)
                ]
                at = pl.multiple_of((4 * g + p) * 2 * length, 2 * length)
                tf[pl.ds(at, 2 * length), :] = pick(moved + [jnp.zeros_like(tiles[0])])
            if st == 1:
                size = 2 * length // groups
                for i in range(rows // 2):
                    lined[i, pl.ds(pl.multiple_of(g * size, size), size)] = row_pair(2 * i, g * 8 * length, size)

        each(0, groups, group)

    await_bytes(uall.at[:, :, pl.ds(0, m - 1)], u_recv)
    own_speed().wait()

    def first_group(g):
        @pl.when(g == 0)
        def _():
            rows_arrive(0)

        @pl.when(g == lower)
        def _():
            rows_arrive(1)

        run_group(0, g)
        for h in range(2):
            keep_own(g, h)

        @pl.when(g < 2)
        def _():
            leave(0, g, g + 1, True)

    each(0, groups, first_group)

    line = lax.broadcasted_iota(jnp.int32, (8, 128), 0)
    largest = jnp.sqrt(jnp.max(peak[...], keepdims=True))
    local_var = jnp.sum(acc[0], keepdims=True) / cells
    local_grad = jnp.sum(acc[1], keepdims=True) / cells
    stat[...] = jnp.where(line == 0, local_var, jnp.where(line == 1, local_grad, largest))
    each(1, n, lambda j: stat_copy((me + j) % n, me).start())
    leave(0, 2, groups, True)
    leave(0, 0, groups, False)
    stats[me] = stat[...]
    rows_sent(0)
    rows_sent(1)
    await_bytes(stats.at[pl.ds(0, n - 1)], t_recv)
    summed = jnp.sum(stats[...], axis=0)
    highest = jnp.max(stats[...], axis=0)
    kappa = ktable[species[0]] * highest[2:3, :1] * jnp.sqrt(summed[0:1, :1]) / (summed[1:2, :1] + 1e-06)
    kap[...] = jnp.broadcast_to(kappa, kap.shape)
    bound = jnp.full((1, half), bounds[0], jnp.int32).astype(f32)
    bound = bound * bound
    rate = -kappa * step_size

    def send_upper(h):
        for kind in uppers:
            each(1, sides, lambda j: block_copy(kind, h, (place + j) % sides, place).start())

    def second(h, c, own, inside):
        block = place + h * sides
        for pr in range(CHUNK // 2):
            r = c * CHUNK + 2 * pr
            moved = dot(fwd_z[...], row_pair(r, 0, 2 * length)) if inside else None
            cols = []
            for k in range(2):
                square = kxz + ky_square(block, r + k)
                factor = jnp.exp(rate * square)
                keep = square <= bound
                for p in range(2):
                    value = tb[h, r + k, p].astype(f32)
                    if inside:
                        add = moved[p * length:(p + 1) * length, k * half:(k + 1) * half]
                        add = jnp.where(keep, -step_size * add, 0.0)
                        value = value + add
                    cols.append((factor * value).astype(bf16))
                    if own:
                        start = out[p, r + k]
                        out[p, r + k] = factor * (start + 0.5 * add) if inside else factor * start
            z_pair(pr, jnp.concatenate(
                [jnp.concatenate(cols[:2], axis=0), jnp.concatenate(cols[2:], axis=0)], axis=1))
        send_rows((2,), h, c)

    def chunks(own, inside):
        h = side if own else 1 - side
        wanted = block_inside(h)

        @pl.when(wanted if inside else jnp.logical_not(wanted))
        def _():
            each(0, nch, lambda c: second(h, c, own, inside))
            if not inside:
                send_upper(h)

    for own in (True, False):
        chunks(own, False)
    for own in (True, False):
        unpack(0, side if own else 1 - side)
        if not own:
            each(1, n, lambda j: pl.semaphore_signal(
                free, inc=1, device_id={"fft": (me + j) % n}, device_id_type=MESH))
        chunks(own, True)

    for h in range(2):
        @pl.when(block_inside(h))
        def _():
            send_upper(h)

    forward_sent(0)

    def last_group(g):
        @pl.when(g == 0)
        def _():
            rows_arrive(2)
            pl.semaphore_wait(free, n - 1)

        @pl.when(g >= lower)
        def _():
            rows_arrive(3 + g - lower)

        run_group(1, g)
        leave(1, g, g + 1, True)
        keep_own(g, side)

    each(0, groups, last_group)
    await_bytes(tb.at[side], x_send)
    await_bytes(uall.at[:, :, pl.ds(0, m - 1)], u_send)
    await_bytes(stats.at[pl.ds(0, n - 1)], t_send)
    for kind in (2, *uppers):
        rows_sent(kind)
    unpack(1, side)
    forward_sent(1)


def final_kernel(rows, length, partial, lined, kap, bounds, fwd_z_in, out, kap_out, fwd_z, done, t_load, d_out):
    half = length // 2
    f32 = jnp.float32
    step_size = cfl_number * 2.0 * math.pi / length
    pairs = rows // 2

    def each(act):
        def one(i, carry):
            act(i)
            return carry

        lax.fori_loop(0, pairs, one, 0, unroll=True)

    def done_copy(i):
        at = pl.ds(2 * i, 2)
        return pltpu.make_async_copy(done.at[:, at], out.at[:, at], d_out.at[i])

    table = pltpu.make_async_copy(fwd_z_in, fwd_z, t_load)
    table.start()

    kx = lax.broadcasted_iota(jnp.int32, (length, half), 1).astype(f32)
    kz = lax.broadcasted_iota(jnp.int32, (length, half), 0)
    kz = jnp.where(kz < half, kz, kz - length).astype(f32)
    bound = jnp.full((1, half), bounds[0], jnp.int32).astype(f32)
    kxz = kx * kx + kz * kz
    kap_out[0] = jnp.max(kap[...])
    table.wait()

    def pair(i):
        moved = dot(fwd_z[...], lined[i])
        for k in range(2):
            ky = lax.axis_index("fft") * rows + i * 2 + k
            ky = jnp.where(ky < half, ky, ky - length)
            keep = kxz + jnp.full((1, half), ky * ky, jnp.int32).astype(f32) <= bound * bound
            for p in range(2):
                value = moved[p * length:(p + 1) * length, k * half:(k + 1) * half]
                done[p, 2 * i + k] = partial[p, 2 * i + k] + jnp.where(keep, -0.5 * step_size * value, 0.0)
        done_copy(i).start()

    each(pair)
    each(lambda i: done_copy(i).wait())


def body(n, m, scalar_state, velocity, species, kappa_table, dealias_bound):
    rows = scalar_state.shape[2]
    length = scalar_state.shape[3]
    half = length // 2
    sides = n // 2
    nch = rows // CHUNK
    groups = rows // 4
    kinds = 4
    f32, bf16 = jnp.float32, jnp.bfloat16
    tables = lax.optimization_barrier(build_tables(length, n, rows))
    vmem = pl.BlockSpec(memory_space=pltpu.VMEM)
    smem = pl.BlockSpec(memory_space=pltpu.SMEM)
    hbm = pl.BlockSpec(memory_space=pl.ANY)
    dma = pltpu.SemaphoreType.DMA
    scratch = [pltpu.VMEM(t.shape, bf16) for t in tables] + [
        pltpu.VMEM((4, length, length), bf16),
        pltpu.VMEM((2, rows, 2, length, half), bf16),
        pltpu.VMEM((2, nch, sides, rows, 2 * CHUNK, 2 * half), bf16),
        pltpu.VMEM((sides, 2, nch, rows, 2 * CHUNK, 2 * half), bf16),
        pltpu.VMEM((2, half * 2 * CHUNK, half), f32),
        pltpu.VMEM((3, rows, m, length // m, length), bf16),
        pltpu.VMEM((n, groups, 3, 2, rows, half), bf16),
        pltpu.VMEM((2, n, groups, 3, 2, rows, half), bf16),
        pltpu.VMEM((2, 2 * length, 2 * half), f32),
        pltpu.VMEM((rows * 2 * length, half), f32),
        pltpu.VMEM((2 * length, 2 * length), bf16),
        pltpu.VMEM((2 * length, 2 * length), bf16),
        pltpu.VMEM((length, length), bf16),
        pltpu.VMEM((8, length), f32),
        pltpu.VMEM((2, 8, half), f32),
        pltpu.VMEM((8, 128), f32),
        pltpu.VMEM((n, 8, 128), f32),
        dma((nch,)), dma((len(tables),)), dma, dma((nch,)), dma((kinds,)), dma((kinds,)), dma, dma, dma,
        dma((2, n)), dma((2, groups, 2)), dma, dma,
        pltpu.SemaphoreType.REGULAR,
    ]
    partial, lined, kappa = pl.pallas_call(
        functools.partial(step_kernel, n, m, rows, length // 3),
        out_shape=[
            pltpu.VMEM((2, rows, length, half), f32),
            pltpu.VMEM((rows // 2, 2 * length, 2 * half), bf16),
            pltpu.VMEM((8, 128), f32),
        ],
        in_specs=[hbm, hbm, smem, smem, smem] + [hbm] * 6,
        out_specs=[vmem, vmem, vmem],
        scratch_shapes=scratch,
        compiler_params=pltpu.CompilerParams(
            collective_id=0, has_side_effects=True, vmem_limit_bytes=56 * 1024 * 1024,
        ),
        name="whole_step",
    )(scalar_state[0], velocity, species, kappa_table, dealias_bound, *tables)
    keep = functools.partial(pltpu.with_memory_space_constraint, memory_space=pltpu.VMEM)
    new_state, kappa = pl.pallas_call(
        functools.partial(final_kernel, rows, length),
        out_shape=[
            jax.ShapeDtypeStruct((2, rows, length, half), f32),
            jax.ShapeDtypeStruct((1,), f32),
        ],
        in_specs=[vmem, vmem, vmem, smem, hbm],
        out_specs=[hbm, smem],
        scratch_shapes=[
            pltpu.VMEM((2 * length, 2 * length), bf16),
            pltpu.VMEM((2, rows, length, half), f32),
            dma, dma((rows // 2,)),
        ],
        compiler_params=pltpu.CompilerParams(vmem_limit_bytes=24 * 1024 * 1024),
        name="final_step",
    )(keep(partial), keep(lined), keep(kappa), dealias_bound, tables[5])
    return new_state[None], kappa


def solution(mesh):
    placed = (
        P("scal", None, "fft", None, None),
        P(None, "fft", "scal", None),
        P("scal"),
        P(),
        P("scal"),
    )
    return jax.shard_map(
        functools.partial(body, mesh.shape["fft"], mesh.shape["scal"]),
        mesh=mesh,
        in_specs=placed,
        out_specs=(P("scal", None, "fft", None, None), P("scal")),
        check_vma=False,
    )
```
